256 devices in a mesh: space: 32 (over x_lo, z, core), spec: 8 (over x_hi, y).
Axes of the slice: x: 4 (x_hi: 2, x_lo: 2; x = x_hi * 2 + x_lo), y: 4, z: 8, core: 2. Of those that a mesh axis runs over, the one named last changes fastest.
Arguments:
- tracers: float32 [240, 8, 256, 384], P('spec', None, 'space'), may hold values from 0.1 to 10
- courant: float32 [2, 8, 256, 384], P(None, None, 'space'), may hold values from -0.9 to 0.9
- layer_mass: float32 [8, 256, 384], P(None, 'space'), may hold values from 0.5 to 2
- pbl_top: int32 [256, 384], P('space'), may hold values from 1 to 8
- land_type: int32 [256, 384], P('space'), may hold values from 0 to 10
- rates: float32 [11, 240], replicated, may hold values from 0.05 to 3
- coupling: float32 [240, 240], replicated, may hold values from -0.375 to 0.375
Outputs:
- updated: float32 [240, 8, 256, 384], P('spec', None, 'space')
- deposited: float32 [240, 256, 384], P('spec', 'space')
The draws below stay inside these ranges and needn't reach their ends.
All inputs are finite; a program needn't handle non-finite values.
Results may differ from the reference program's by a relative error of at most 0.0003.
Values sent between devices are 32-bit elements; how exact they have to be, the bound alone decides.
No kernel may reach another device: no remote copies, remote signals or barrier semaphores. Data moves between devices by JAX's collectives and lax.ppermute only.
A program may use at most 128 MiB of HBM per device.

```python
import math
import jax
import jax.numpy as jnp
from jax import lax

SPECIES = 240
LEVELS = 8
LAND = 11
STEPS = 2
NY = 384
NX = 256
N_SPEC = 8


def place_ends(entries, key, low, top_value):
    dims = entries.shape
    spot = [jax.random.randint(jax.random.fold_in(key, axis), (), 0, dims[axis]) for axis in range(len(dims))]
    entries = entries.at[tuple(spot)].set(low)
    longest = dims.index(max(dims))
    spot[longest] = (spot[longest] + 1) % dims[longest]
    return entries.at[tuple(spot)].set(top_value)


def level_of(own_key, shape, shards, low, high):
    factor_of, own = 1.0, jax.random.fold_in(own_key, 6)
    for dim, shards_of in shards:
        draws = jnp.exp(jax.random.uniform(jax.random.fold_in(own, dim), (shards_of,), jnp.float32, low / len(shards), high / len(shards)))
        factor_of = factor_of * jnp.repeat(draws, shape[dim] // shards_of).reshape([-1 if axis == dim else 1 for axis in range(len(shape))])
    return factor_of


def centred(rng, extent, spread, bound, held_as=jnp.bfloat16):
    result = jax.random.normal(rng, extent, jnp.float32) * spread
    return jnp.minimum(jnp.maximum(result, -bound), bound).astype(held_as)


def setup_inputs(seed: int = 0) -> dict:
    splits = jax.random.split(jax.random.key(seed), 8)
    return {
        "tracers": jnp.clip(jnp.exp(math.log(10.0) - 4.6051702 * jax.random.uniform(splits[0], (SPECIES, LEVELS, NX, NY), jnp.float32) ** level_of(splits[0], (SPECIES, LEVELS, NX, NY), ((0, 8), (2, 32)), -0.2, 0.2)), 0.1, 10.0),
        "courant": jnp.clip(jax.random.uniform(splits[1], (2, LEVELS, NX, NY), jnp.float32, -0.9, 0.9) * level_of(splits[1], (2, LEVELS, NX, NY), ((2, 32),), -0.4, 0.0), -0.9, 0.9),
        "layer_mass": jnp.clip(jnp.exp(math.log(2.0) - 1.3862944 * jax.random.uniform(splits[2], (LEVELS, NX, NY), jnp.float32) ** level_of(splits[2], (LEVELS, NX, NY), ((1, 32),), -0.2, 0.2)), 0.5, 2.0),
        "pbl_top": place_ends(jax.random.randint(splits[3], (NX, NY), 1, LEVELS + 1), jax.random.fold_in(splits[3], 1), 1, LEVELS).astype(jnp.int32),
        "land_type": place_ends(jax.random.randint(splits[4], (NX, NY), 0, LAND), jax.random.fold_in(splits[4], 1), 0, LAND - 1).astype(jnp.int32),
        "rates": jnp.clip(jnp.exp(jax.random.uniform(splits[5], (LAND, SPECIES), jnp.float32, math.log(0.05), math.log(3.0))), 0.05, 3.0),
        "coupling": centred(splits[6], (SPECIES, SPECIES), SPECIES ** -0.5, 0.375, jnp.float32),
    }


def sweep(field, speed, axis):
    count = field.shape[axis]

    def cut(a, lo, hi):
        return lax.slice_in_dim(a, lo, hi, axis=axis)

    edge = (7.0 / 12.0) * (cut(field, 1, count - 2) + cut(field, 2, count - 1)) - (1.0 / 12.0) * (cut(field, 0, count - 3) + cut(field, 3, count))
    lower = cut(edge, 0, count - 4)
    upper = cut(edge, 1, count - 3)
    centre = cut(field, 2, count - 2)
    slope = upper - lower
    curve = 6.0 * (centre - 0.5 * (lower + upper))
    cells = count - 4
    face = cut(speed, 3, count - 2)
    upwind = face * (cut(upper, 0, cells - 1) - 0.5 * face * (cut(slope, 0, cells - 1) - (1.0 - 2.0 * face / 3.0) * cut(curve, 0, cells - 1)))
    downwind = face * (cut(lower, 1, cells) - 0.5 * face * (cut(slope, 1, cells) + (1.0 + 2.0 * face / 3.0) * cut(curve, 1, cells)))
    flux = jnp.where(face >= 0.0, upwind, downwind)
    return cut(field, 3, count - 3) - (cut(flux, 1, count - 5) - cut(flux, 0, count - 6))


def advect(block, courant):
    for step in range(STEPS):
        padded = jnp.pad(block, ((0, 0), (0, 0), (3, 3), (0, 0)))
        speed = jnp.pad(courant[0], ((0, 0), (3, 3), (0, 0)))
        block = sweep(padded, speed, -2)
        padded = jnp.pad(block, ((0, 0), (0, 0), (0, 0), (3, 3)))
        speed = jnp.pad(courant[1], ((0, 0), (0, 0), (3, 3)))
        block = sweep(padded, speed, -1)
    return block


def mixing(field, layer_mass, pbl_top):
    levels = jnp.arange(field.shape[1], dtype=jnp.int32)[:, None, None]
    inside = levels < pbl_top[None]
    weights = jnp.where(inside, layer_mass, 0.0)
    average = jnp.sum(weights[None] * field, axis=1) / jnp.sum(weights, axis=0)[None]
    return jnp.where(inside[None], average[:, None], field)


def deposit(field, surface_mass, land_type, rates):
    kinds = jnp.arange(rates.shape[0], dtype=jnp.int32)[:, None]
    onehot = (land_type.reshape(1, -1) == kinds).astype(jnp.float32)
    loss = jnp.dot(rates.T, onehot, precision=lax.Precision.HIGHEST).reshape(field.shape[0], field.shape[2], field.shape[3])
    bottom = field[:, 0]
    kept = bottom * jnp.exp(-loss)
    return field.at[:, 0].set(kept), (bottom - kept) * surface_mass[None]


def reference(tracers, courant, layer_mass, pbl_top, land_type, rates, coupling):
    groups = tracers.reshape(N_SPEC, SPECIES // N_SPEC, LEVELS, NX, NY)
    advected = lax.map(lambda block: advect(block, courant), groups).reshape(SPECIES, LEVELS, NX, NY)
    mixed = mixing(advected, layer_mass, pbl_top)
    coupled = mixed + jnp.dot(coupling, mixed.reshape(SPECIES, -1), precision=lax.Precision.HIGHEST).reshape(mixed.shape)
    updated, deposited = deposit(coupled, layer_mass[0], land_type, rates)
    return updated, deposited
```

```python
import functools

import jax
import jax.numpy as jnp
from jax import lax
from jax.experimental import pallas as pl
from jax.experimental.pallas import tpu as pltpu
from jax.sharding import PartitionSpec as P

INTERPRET = False
F32 = jnp.float32
BF16 = jnp.bfloat16
TAPS = 7
HALO = 6


def call(body, out_shape, **kw):
    return pl.pallas_call(body, out_shape=out_shape, interpret=INTERPRET, **kw)


def pack_even(x, cf, own, up, down, speeds):
    tiles = own.shape[1] // 8
    width = own.shape[1]
    for r in range(8):
        for i in range(tiles):
            value = x[pl.ds(i * 128 + r, 8, stride=16), :]
            own[r, i * 8 : i * 8 + 8, :] = value
            if r >= 2:
                at = (r - 2) * width + i * 8
                up[at : at + 8, :] = value
            if r < 6:
                at = r * width + i * 8
                down[at : at + 8, :] = value
    for d in range(2):
        for parity in range(2):
            for row in range(4):
                at = HALO * width + ((d * 2 + parity) * 4 + row) * 4
                start = d * 64 + parity * 8 + row
                before = cf[pl.ds(start, 4, stride=16), :]
                after = cf[pl.ds(start + 4, 4, stride=16), :]
                down[at : at + 4, :] = before
                up[at : at + 4, :] = after
                for half in (slice(0, 4), slice(4, 8)):
                    speeds[parity, d, row, half, :] = before
                    speeds[parity, d, row + 4, half, :] = after


def pack_odd(x, own):
    for r in range(8):
        for i in range(own.shape[1] // 8):
            own[r, i * 8 : i * 8 + 8, :] = x[pl.ds(i * 128 + 8 + r, 8, stride=16), :]


def flux_taps(c):
    u = jnp.abs(c)
    square = u * u
    edge = c * (1.0 - u) * (1.0 - u)
    other = square * (1.0 - u)
    centre = square * (3.0 - 2.0 * u)
    ahead = c >= 0.0
    below = jnp.where(ahead, -other, 0.0)
    above = jnp.where(ahead, 0.0, other)
    lower = jnp.where(ahead, centre, 0.0)
    upper = jnp.where(ahead, 0.0, -centre)
    a, b = 7.0 / 12.0, 1.0 / 12.0
    return (
        -b * below,
        a * below - b * edge,
        a * (edge + below) - b * above + lower,
        a * (edge + above) - b * below + upper,
        a * above - b * edge,
        -b * above,
    )


def cell_taps(low, high):
    return (
        low[0],
        low[1] - high[0],
        low[2] - high[1],
        1.0 + low[3] - high[2],
        low[4] - high[3],
        low[5] - high[4],
        -high[5],
    )


def transport(parity, own, up, down, cup, cdown, cf, valid, out, c, wx, wy, mid):
    width = own.shape[1]
    ny = own.shape[2]
    for d in range(2):
        c[d, 4:12] = cf[parity, d]
        for row in range(4):
            at = ((d * 2 + parity) * 4 + row) * 4
            for half in (slice(0, 4), slice(4, 8)):
                c[d, row, half, :] = cup[at : at + 4, :]
                c[d, row + 12, half, :] = cdown[at : at + 4, :]
    lane = lax.broadcasted_iota(jnp.int32, (8, ny), 1)
    inside = valid[0, 0]
    for t in range(ny // 128):
        cols = slice(t * 128, t * 128 + 128)
        high = flux_taps(c[0, 1, :, cols])
        for row in range(14):
            low, high = high, flux_taps(c[0, row + 2, :, cols])
            for k, w in enumerate(cell_taps(low, high)):
                wx[row, k, :, cols] = w * inside if row < 3 else w

    def y_weights(row, carry):
        speed = c[1, row + 1]
        low = flux_taps(speed)
        high = flux_taps(jnp.where(lane == ny - 1, 0.0, pltpu.roll(speed, ny - 1, 1)))
        for k, w in enumerate(cell_taps(low, high)):
            shift = k - 3
            w = jnp.where((lane + shift >= 0) & (lane + shift < ny), w, 0.0)
            wy[row, k] = w
        return carry

    lax.fori_loop(0, 14, y_weights, 0)

    def across(value, row):
        total = wy[row, 3] * value
        for shift in (1, 2, 3):
            total += wy[row, 3 + shift] * pltpu.roll(value, ny - shift, 1)
            total += wy[row, 3 - shift] * pltpu.roll(value, shift, 1)
        return total

    def tile(i, carry):
        at = pl.multiple_of(i * 8, 8)

        def first(row, cols):
            if row < 0:
                return up[pl.ds((row + HALO) * width + at, 8), cols]
            if row < 8:
                return own[row, pl.ds(at, 8), cols]
            return down[pl.ds((row - 8) * width + at, 8), cols]

        def along(read, row):
            parts = []
            for t in range(ny // 128):
                cols = slice(t * 128, t * 128 + 128)
                total = wx[row + 3, 0, :, cols] * read(row - 3, cols)
                for k in range(1, TAPS):
                    total += wx[row + 3, k, :, cols] * read(row + k - 3, cols)
                parts.append(total)
            return jnp.concatenate(parts, axis=1)

        for row in range(-3, 11):
            mid[row + 3] = across(along(first, row), row + 3)
        for row in range(8):
            value = along(lambda at_row, cols: mid[at_row + 3, :, cols], row)
            out[row, pl.ds(at, 8), :] = across(value, row + 3)
        return carry

    lax.fori_loop(0, width // 8, tile, 0)


def halves(value):
    top = value.astype(BF16)
    return top, (value - top.astype(F32)).astype(BF16)


def couple(x, matrix, out, wide):
    species = matrix.shape[0]
    for j in range(4):
        wide[:, j * 128 : j * 128 + 128] = x[pl.ds(j, species, stride=4), :]
    value = wide[...]
    top, rest = halves(value)
    high, low = halves(matrix[...])
    total = jnp.dot(high, top, preferred_element_type=F32)
    total += jnp.dot(high, rest, preferred_element_type=F32)
    total += jnp.dot(low, top, preferred_element_type=F32)
    wide[...] = value + total
    for j in range(4):
        out[pl.ds(j, species, stride=4), :] = wide[:, j * 128 : j * 128 + 128]


def prepare(lm, pbl, land, rates, keep, weven, wodd):
    ny = lm.shape[1]
    kinds = lax.broadcasted_iota(jnp.int32, (rates.shape[1], ny), 0)
    levels = lax.broadcasted_iota(jnp.int32, (8, ny), 0)
    evens = 2 * lax.broadcasted_iota(jnp.int32, (4, ny), 0)
    for r in range(8):
        top = pbl[r : r + 1, :]
        mass = lm[pl.ds(r, 8, stride=8), :]
        total = jnp.sum(jnp.where(levels < top, mass, 0.0), axis=0, keepdims=True)
        scale = 1.0 / total
        even = jnp.where(evens < top, lm[pl.ds(r, 4, stride=16), :], 0.0) * scale
        odd = jnp.where(evens + 1 < top, lm[pl.ds(8 + r, 4, stride=16), :], 0.0) * scale
        weven[r, 0:4, :] = even
        weven[r, 4:8, :] = even
        wodd[r, 0:4, :] = odd
        wodd[r, 4:8, :] = odd
        onehot = (kinds == land[r : r + 1, :]).astype(F32)
        loss = jnp.dot(
            rates[...], onehot, precision=lax.Precision.HIGHEST, preferred_element_type=F32
        )
        keep[r] = jnp.exp(-loss)


def finish(even, odd, keep, weven, wodd, pbl, lm, out, dep, flux):
    ny = even.shape[2]
    sub = lax.broadcasted_iota(jnp.int32, (8, ny), 0)
    level = 2 * (sub % 4)
    first = sub % 2 == 0
    low = sub % 4 < 2
    for r in range(8):
        top = pbl[r : r + 1, :]
        for i in range(even.shape[1] // 8):
            at = slice(i * 8, i * 8 + 8)
            a, b = even[r, at, :], odd[r, at, :]
            total = weven[r] * a + wodd[r] * b
            total += jnp.where(first, pltpu.roll(total, 7, 0), pltpu.roll(total, 1, 0))
            total += jnp.where(low, pltpu.roll(total, 6, 0), pltpu.roll(total, 2, 0))
            a = jnp.where(level < top, total, a)
            b = jnp.where(level + 1 < top, total, b)
            kept = a * keep[r, at, :]
            flux[at, :] = (a - kept) * lm[r : r + 1, :]
            out[pl.ds(i * 128 + r, 8, stride=16), :] = kept
            out[pl.ds(i * 128 + 8 + r, 8, stride=16), :] = b
        count = even.shape[1] // 4
        dep[pl.ds(r, count, stride=8), :] = flux[pl.ds(0, count, stride=4), :]


def on_device(tracers, courant, layer_mass, pbl_top, land_type, rates, coupling):
    own_species, levels, rows, ny = tracers.shape
    species = coupling.shape[0]
    width = own_species * 4
    sds = jax.ShapeDtypeStruct
    n_space, n_spec = lax.axis_size("space"), lax.axis_size("spec")
    up_pairs = [(i, i + 1) for i in range(n_space - 1)]
    down_pairs = [(j, i) for i, j in up_pairs]
    flat = tracers.reshape(-1, ny)
    cf = courant.reshape(-1, ny)
    lm = layer_mass.reshape(-1, ny)
    valid = (lax.axis_index("space") > 0).astype(F32).reshape(1, 1)

    group = sds((rows, width, ny), F32)
    edge = sds((HALO * width + 64, ny), F32)
    speeds = sds((2, 2, rows, 8, ny), F32)
    strips = ny // 128

    def strip(*shape):
        return pl.BlockSpec((*shape, 128), lambda t: (0,) * len(shape) + (t,))

    even, send_up, send_down, speeds = call(
        pack_even,
        (group, edge, edge, speeds),
        grid=(strips,),
        in_specs=[strip(flat.shape[0]), strip(cf.shape[0])],
        out_specs=[
            strip(rows, width),
            strip(edge.shape[0]),
            strip(edge.shape[0]),
            strip(2, 2, rows, 8),
        ],
    )(flat, cf)
    up = lax.ppermute(send_up, "space", up_pairs)
    down = lax.ppermute(send_down, "space", down_pairs)
    odd = call(
        pack_odd,
        group,
        grid=(strips,),
        in_specs=[strip(flat.shape[0])],
        out_specs=strip(rows, width),
    )(flat)

    def exchange(a):
        return lax.all_to_all(a, "spec", split_axis=0, concat_axis=0, tiled=True)

    def coupled(a):
        block = strip(species * 4)
        whole = pl.BlockSpec((species, species), lambda t: (0, 0))
        got = call(
            couple,
            sds((species * 4, ny), F32),
            grid=(strips,),
            in_specs=[block, whole],
            out_specs=block,
            scratch_shapes=[pltpu.VMEM((species, 512), F32)],
        )(a.reshape(species * 4, ny), coupling)
        return got.reshape(a.shape)

    cup, cdown = up[HALO * width :], down[HALO * width :]

    def transported(parity, a, before, after):
        vmem = pl.BlockSpec(memory_space=pltpu.VMEM)
        return call(
            functools.partial(transport, parity),
            group,
            in_specs=[vmem] * 6 + [pl.BlockSpec(memory_space=pltpu.SMEM)],
            out_specs=vmem,
            scratch_shapes=[
                pltpu.VMEM((2, 16, 8, ny), F32),
                pltpu.VMEM((14, TAPS, 8, ny), F32),
                pltpu.VMEM((14, TAPS, 8, ny), F32),
                pltpu.VMEM((14, 8, ny), F32),
            ],
        )(a, before, after, cup, cdown, speeds, valid)

    start = lax.axis_index("spec") * own_species
    mine = lax.dynamic_slice_in_dim(rates, start, own_species, 1).T
    kinds = mine.shape[1]
    mine = jnp.pad(mine[:, None], ((0, 0), (0, 3), (0, 16 - kinds))).reshape(width, 16)
    tile = sds((rows, 8, ny), F32)
    keep, weven, wodd = call(
        prepare,
        (group, tile, tile),
        grid=(strips,),
        in_specs=[
            strip(lm.shape[0]),
            strip(rows),
            strip(rows),
            pl.BlockSpec(mine.shape, lambda t: (0, 0)),
        ],
        out_specs=[strip(rows, width), strip(rows, 8), strip(rows, 8)],
    )(lm, pbl_top, land_type, mine)

    odd = exchange(odd)
    even = transported(0, even, up, down)
    even = exchange(even)
    odd = exchange(coupled(odd))
    even = exchange(coupled(even))
    up = lax.ppermute(odd[2:].reshape(-1, ny), "space", up_pairs)
    down = lax.ppermute(odd[:HALO].reshape(-1, ny), "space", down_pairs)
    odd = transported(1, odd, up, down)

    part = 24
    block = pl.BlockSpec((rows, part, 128), lambda i, t: (0, i, t))
    fixed = pl.BlockSpec((rows, 8, 128), lambda i, t: (0, 0, t))
    plane = pl.BlockSpec((rows, 128), lambda i, t: (0, t))
    updated, deposited = call(
        finish,
        (sds(flat.shape, F32), sds((own_species * rows, ny), F32)),
        grid=(width // part, strips),
        in_specs=[block, block, block, fixed, fixed, plane, plane],
        out_specs=[
            pl.BlockSpec((part * 16, 128), lambda i, t: (i, t)),
            pl.BlockSpec((part * 2, 128), lambda i, t: (i, t)),
        ],
        scratch_shapes=[pltpu.VMEM((part, 128), F32)],
    )(even, odd, keep, weven, wodd, pbl_top, lm)
    return (updated.reshape(tracers.shape), deposited.reshape(own_species, rows, ny))


def solution(mesh):
    return jax.shard_map(
        on_device,
        mesh=mesh,
        in_specs=(
            P("spec", None, "space", None),
            P(None, None, "space", None),
            P(None, "space", None),
            P("space", None),
            P("space", None),
            P(),
            P(),
        ),
        out_specs=(P("spec", None, "space", None), P("spec", "space", None)),
        check_vma=False,
    )
```

```python
import functools

import jax
import jax.numpy as jnp
from jax import lax
from jax.experimental import pallas as pl
from jax.experimental.pallas import tpu as pltpu
from jax.sharding import PartitionSpec as P

INTERPRET = False
F32 = jnp.float32
BF16 = jnp.bfloat16
TAPS = 7
HALO = 6


def call(body, out_shape, **kw):
    return pl.pallas_call(body, out_shape=out_shape, interpret=INTERPRET, **kw)


def pack_even(x, cf, own, up, down, speeds):
    width = own.shape[1]
    x = x.reshape(width * 8, 128)
    for r in range(8):
        for i in range(width // 8):
            value = x[pl.ds(i * 64 + r, 8, stride=8), :]
            own[r, i * 8 : i * 8 + 8, :] = value
            if r >= 2:
                at = (r - 2) * width + i * 8
                up[at : at + 8, :] = value
            if r < 6:
                at = r * width + i * 8
                down[at : at + 8, :] = value
    for d in range(2):
        for parity in range(2):
            for row in range(4):
                at = HALO * width + ((d * 2 + parity) * 4 + row) * 4
                start = d * 64 + parity * 8 + row
                before = cf[pl.ds(start, 4, stride=16), :]
                after = cf[pl.ds(start + 4, 4, stride=16), :]
                down[at : at + 4, :] = before
                up[at : at + 4, :] = after
                for half in (slice(0, 4), slice(4, 8)):
                    speeds[parity, d, row, half, :] = before
                    speeds[parity, d, row + 4, half, :] = after


def pack_odd(x, own):
    x = x.reshape(own.shape[1] * 8, 128)
    for r in range(8):
        for i in range(own.shape[1] // 8):
            own[r, i * 8 : i * 8 + 8, :] = x[pl.ds(i * 64 + r, 8, stride=8), :]


def flux_taps(c):
    u = jnp.abs(c)
    square = u * u
    edge = c * (1.0 - u) * (1.0 - u)
    other = square * (1.0 - u)
    centre = square * (3.0 - 2.0 * u)
    ahead = c >= 0.0
    below = jnp.where(ahead, -other, 0.0)
    above = jnp.where(ahead, 0.0, other)
    lower = jnp.where(ahead, centre, 0.0)
    upper = jnp.where(ahead, 0.0, -centre)
    a, b = 7.0 / 12.0, 1.0 / 12.0
    return (
        -b * below,
        a * below - b * edge,
        a * (edge + below) - b * above + lower,
        a * (edge + above) - b * below + upper,
        a * above - b * edge,
        -b * above,
    )


def cell_taps(low, high):
    return (
        low[0],
        low[1] - high[0],
        low[2] - high[1],
        1.0 + low[3] - high[2],
        low[4] - high[3],
        low[5] - high[4],
        -high[5],
    )


def transport(parity, own, up, down, cup, cdown, cf, valid, out, c, wx, wy, mid):
    width = own.shape[2]
    ny = own.shape[3]
    for d in range(2):
        c[d, 4:12] = cf[parity, d]
        for row in range(4):
            at = ((d * 2 + parity) * 4 + row) * 4
            for half in (slice(0, 4), slice(4, 8)):
                c[d, row, half, :] = cup[at : at + 4, :]
                c[d, row + 12, half, :] = cdown[at : at + 4, :]
    lane = lax.broadcasted_iota(jnp.int32, (8, ny), 1)
    inside = valid[0, 0]
    for t in range(ny // 128):
        cols = slice(t * 128, t * 128 + 128)
        high = flux_taps(c[0, 1, :, cols])
        for row in range(14):
            low, high = high, flux_taps(c[0, row + 2, :, cols])
            for k, w in enumerate(cell_taps(low, high)):
                wx[row, k, :, cols] = w * inside if row < 3 else w

    def y_weights(row, carry):
        speed = c[1, row + 1]
        low = flux_taps(speed)
        high = flux_taps(jnp.where(lane == ny - 1, 0.0, pltpu.roll(speed, ny - 1, 1)))
        for k, w in enumerate(cell_taps(low, high)):
            shift = k - 3
            w = jnp.where((lane + shift >= 0) & (lane + shift < ny), w, 0.0)
            wy[row, k] = w
        return carry

    lax.fori_loop(0, 14, y_weights, 0)

    group = range(3)

    def across(values, row):
        w = wy[row, 3]
        totals = [w * v for v in values]
        for shift in (1, 2, 3):
            w = wy[row, 3 + shift]
            totals = [t + w * pltpu.roll(v, ny - shift, 1) for t, v in zip(totals, values)]
            w = wy[row, 3 - shift]
            totals = [t + w * pltpu.roll(v, shift, 1) for t, v in zip(totals, values)]
        return totals

    def tile(i, carry):
        places = [pl.multiple_of(i * 24 + 8 * u, 8) for u in group]

        def first(row, cols, u):
            at = places[u]
            if row < 0:
                return up[pl.ds((row + HALO) * width + at, 8), cols]
            if row < 8:
                return own[row, 0, pl.ds(at, 8), cols]
            return down[pl.ds((row - 8) * width + at, 8), cols]

        def second(row, cols, u):
            return mid[row + 3, u, :, cols]

        def along(read, row):
            parts = [[] for _ in group]
            for t in range(ny // 128):
                cols = slice(t * 128, t * 128 + 128)
                w = wx[row + 3, 0, :, cols]
                totals = [w * read(row - 3, cols, u) for u in group]
                for k in range(1, TAPS):
                    w = wx[row + 3, k, :, cols]
                    totals = [v + w * read(row + k - 3, cols, u) for u, v in enumerate(totals)]
                for part, v in zip(parts, totals):
                    part.append(v)
            return [jnp.concatenate(part, axis=1) for part in parts]

        for row in range(-3, 11):
            for u, v in enumerate(across(along(first, row), row + 3)):
                mid[row + 3, u] = v
        for row in range(8):
            for u, v in enumerate(across(along(second, row), row + 3)):
                out[row, 0, pl.ds(places[u], 8), :] = v
        return carry

    lax.fori_loop(0, width // 24, tile, 0)


def halves(value):
    top = value.astype(BF16)
    return top, (value - top.astype(F32)).astype(BF16)


def couple(x, matrix, *refs):
    out, wide = refs[-2:]
    species = matrix.shape[0]
    x = x.reshape(species * 4, 128)
    out = out.reshape(species * 4, 128)
    for j in range(4):
        wide[:, j * 128 : j * 128 + 128] = x[pl.ds(j, species, stride=4), :]
    value = wide[...]
    top, rest = halves(value)
    high, low = halves(matrix[...])
    total = jnp.dot(high, top, preferred_element_type=F32)
    total += jnp.dot(high, rest, preferred_element_type=F32)
    total += jnp.dot(low, top, preferred_element_type=F32)
    wide[...] = value + total
    for j in range(4):
        out[pl.ds(j, species, stride=4), :] = wide[:, j * 128 : j * 128 + 128]


def prepare(lm, pbl, land, rates, keep, weven, wodd):
    ny = lm.shape[1]
    kinds = lax.broadcasted_iota(jnp.int32, (rates.shape[1], ny), 0)
    levels = lax.broadcasted_iota(jnp.int32, (8, ny), 0)
    evens = 2 * lax.broadcasted_iota(jnp.int32, (4, ny), 0)
    for r in range(8):
        top = pbl[r : r + 1, :]
        mass = lm[pl.ds(r, 8, stride=8), :]
        total = jnp.sum(jnp.where(levels < top, mass, 0.0), axis=0, keepdims=True)
        scale = 1.0 / total
        even = jnp.where(evens < top, lm[pl.ds(r, 4, stride=16), :], 0.0) * scale
        odd = jnp.where(evens + 1 < top, lm[pl.ds(8 + r, 4, stride=16), :], 0.0) * scale
        weven[r, 0:4, :] = even
        weven[r, 4:8, :] = even
        wodd[r, 0:4, :] = odd
        wodd[r, 4:8, :] = odd
        onehot = (kinds == land[r : r + 1, :]).astype(F32)
        loss = jnp.dot(
            rates[...], onehot, precision=lax.Precision.HIGHEST, preferred_element_type=F32
        )
        keep[r] = jnp.exp(-loss)


def finish(even, odd, keep, weven, wodd, pbl, lm, out, dep, flux):
    ny = even.shape[2]
    sub = lax.broadcasted_iota(jnp.int32, (8, ny), 0)
    level = 2 * (sub % 4)
    first = sub % 2 == 0
    low = sub % 4 < 2
    for r in range(8):
        top = pbl[r : r + 1, :]
        for i in range(even.shape[1] // 8):
            at = slice(i * 8, i * 8 + 8)
            a, b = even[r, at, :], odd[r, at, :]
            total = weven[r] * a + wodd[r] * b
            total += jnp.where(first, pltpu.roll(total, 7, 0), pltpu.roll(total, 1, 0))
            total += jnp.where(low, pltpu.roll(total, 6, 0), pltpu.roll(total, 2, 0))
            a = jnp.where(level < top, total, a)
            b = jnp.where(level + 1 < top, total, b)
            kept = a * keep[r, at, :]
            flux[at, :] = (a - kept) * lm[r : r + 1, :]
            out[pl.ds(i * 128 + r, 8, stride=16), :] = kept
            out[pl.ds(i * 128 + 8 + r, 8, stride=16), :] = b
        count = even.shape[1] // 4
        dep[pl.ds(r, count, stride=8), :] = flux[pl.ds(0, count, stride=4), :]


def on_device(tracers, courant, layer_mass, pbl_top, land_type, rates, coupling):
    own_species, levels, rows, ny = tracers.shape
    species = coupling.shape[0]
    width = own_species * 4
    sds = jax.ShapeDtypeStruct
    n_space, n_spec = lax.axis_size("space"), lax.axis_size("spec")
    up_pairs = [(i, i + 1) for i in range(n_space - 1)]
    down_pairs = [(j, i) for i, j in up_pairs]
    split = tracers.reshape(own_species, 4, 2, rows, ny)
    cf = courant.reshape(-1, ny)
    lm = layer_mass.reshape(-1, ny)
    valid = (lax.axis_index("space") > 0).astype(F32).reshape(1, 1)

    group = sds((rows, width, ny), F32)
    edge = sds((HALO * width + 64, ny), F32)
    speeds = sds((2, 2, rows, 8, ny), F32)
    strips = ny // 128

    def strip(*shape):
        return pl.BlockSpec((*shape, 128), lambda t: (0,) * len(shape) + (t,))

    def level_group(parity):
        shape = (own_species, 4, 1, rows, 128)
        return pl.BlockSpec(shape, lambda t: (0, 0, parity, 0, t))

    even, send_up, send_down, speeds = call(
        pack_even,
        (group, edge, edge, speeds),
        grid=(strips,),
        in_specs=[level_group(0), strip(cf.shape[0])],
        out_specs=[
            strip(rows, width),
            strip(edge.shape[0]),
            strip(edge.shape[0]),
            strip(2, 2, rows, 8),
        ],
    )(split, cf)
    up = lax.ppermute(send_up, "space", up_pairs)
    down = lax.ppermute(send_down, "space", down_pairs)
    odd = call(
        pack_odd,
        group,
        grid=(strips,),
        in_specs=[level_group(1)],
        out_specs=strip(rows, width),
    )(split)

    def exchange(a):
        return lax.all_to_all(a, "spec", split_axis=0, concat_axis=0, tiled=True)

    pair = sds((rows, 2, width, ny), F32)

    def half(index):
        return pl.BlockSpec((rows, 1, width, 128), lambda t: (0, index, 0, t))

    def coupled(a, index, shape, out_index, *into):
        whole = pl.BlockSpec((species, species), lambda t: (0, 0))
        return call(
            couple,
            shape,
            grid=(strips,),
            in_specs=[half(index), whole] + [pl.BlockSpec(memory_space=pl.ANY)] * len(into),
            out_specs=half(out_index),
            scratch_shapes=[pltpu.VMEM((species, 512), F32)],
            input_output_aliases={2: 0} if into else {},
        )(a, coupling, *into)

    cup, cdown = up[HALO * width :], down[HALO * width :]

    def transported(parity, a, index, shape, before, after):
        def plane(i):
            return pl.BlockSpec((rows, 1, width, ny), lambda t: (0, i, 0, 0))

        def whole(array):
            return pl.BlockSpec(array.shape, lambda t: (0,) * array.ndim)

        return call(
            functools.partial(transport, parity),
            shape,
            grid=(1,),
            in_specs=[plane(index)]
            + [whole(v) for v in (before, after, cup, cdown, speeds)]
            + [pl.BlockSpec(memory_space=pltpu.SMEM)],
            out_specs=plane(0),
            scratch_shapes=[
                pltpu.VMEM((2, 16, 8, ny), F32),
                pltpu.VMEM((14, TAPS, 8, ny), F32),
                pltpu.VMEM((14, TAPS, 8, ny), F32),
                pltpu.VMEM((14, 3, 8, ny), F32),
            ],
        )(a, before, after, cup, cdown, speeds, valid)

    start = lax.axis_index("spec") * own_species
    mine = lax.dynamic_slice_in_dim(rates, start, own_species, 1).T
    kinds = mine.shape[1]
    mine = jnp.pad(mine[:, None], ((0, 0), (0, 3), (0, 16 - kinds))).reshape(width, 16)
    tile = sds((rows, 8, ny), F32)
    keep, weven, wodd = call(
        prepare,
        (group, tile, tile),
        grid=(strips,),
        in_specs=[
            strip(lm.shape[0]),
            strip(rows),
            strip(rows),
            pl.BlockSpec(mine.shape, lambda t: (0, 0)),
        ],
        out_specs=[strip(rows, width), strip(rows, 8), strip(rows, 8)],
    )(lm, pbl_top, land_type, mine)

    single = sds((rows, 1, width, ny), F32)
    odd = exchange(odd)
    both = transported(0, even[:, None], 0, pair, up, down)
    both = coupled(odd[:, None], 0, pair, 1, both)
    both = exchange(both)
    even = exchange(coupled(both, 0, single, 0))[:, 0]
    up = lax.ppermute(both[2:, 1].reshape(-1, ny), "space", up_pairs)
    down = lax.ppermute(both[:HALO, 1].reshape(-1, ny), "space", down_pairs)
    odd = transported(1, both, 1, single, up, down)[:, 0]

    updated, deposited = call(
        finish,
        (sds((tracers.size // ny, ny), F32), sds((own_species * rows, ny), F32)),
        grid=(strips,),
        in_specs=[strip(rows, width)] * 3 + [strip(rows, 8)] * 2 + [strip(rows)] * 2,
        out_specs=[strip(tracers.size // ny), strip(own_species * rows)],
        scratch_shapes=[pltpu.VMEM((width, 128), F32)],
    )(even, odd, keep, weven, wodd, pbl_top, lm)
    return (updated.reshape(tracers.shape), deposited.reshape(own_species, rows, ny))


def solution(mesh):
    return jax.shard_map(
        on_device,
        mesh=mesh,
        in_specs=(
            P("spec", None, "space", None),
            P(None, None, "space", None),
            P(None, "space", None),
            P("space", None),
            P("space", None),
            P(),
            P(),
        ),
        out_specs=(P("spec", None, "space", None), P("spec", "space", None)),
        check_vma=False,
    )
```

```python
import functools

import jax
import jax.numpy as jnp
from jax import lax
from jax.experimental import pallas as pl
from jax.experimental.pallas import tpu as pltpu
from jax.sharding import PartitionSpec as P


INTERPRET = False
F32 = jnp.float32
BF16 = jnp.bfloat16
TAPS = 7
HALO = 6


def call(body, out_shape, **kw):
    return pl.pallas_call(body, out_shape=out_shape, interpret=INTERPRET, **kw)


def pack_even(x, cf, own, up, down, speeds):
    width = own.shape[1]
    x = x.reshape(width * 8, 128)
    for r in range(8):
        for i in range(width // 8):
            value = x[pl.ds(i * 64 + r, 8, stride=8), :]
            own[r, i * 8 : i * 8 + 8, :] = value
            if r >= 2:
                at = (r - 2) * width + i * 8
                up[at : at + 8, :] = value
            if r < 6:
                at = r * width + i * 8
                down[at : at + 8, :] = value
    for d in range(2):
        for parity in range(2):
            for row in range(4):
                at = HALO * width + ((d * 2 + parity) * 4 + row) * 4
                start = d * 64 + parity * 8 + row
                before = cf[pl.ds(start, 4, stride=16), :]
                after = cf[pl.ds(start + 4, 4, stride=16), :]
                down[at : at + 4, :] = before
                up[at : at + 4, :] = after
                for half in (slice(0, 4), slice(4, 8)):
                    speeds[parity, d, row, half, :] = before
                    speeds[parity, d, row + 4, half, :] = after


def pack_odd(x, own):
    x = x.reshape(own.shape[1] * 8, 128)
    for r in range(8):
        for i in range(own.shape[1] // 8):
            own[r, i * 8 : i * 8 + 8, :] = x[pl.ds(i * 64 + r, 8, stride=8), :]


def flux_taps(c):
    u = jnp.abs(c)
    square = u * u
    edge = c * (1.0 - u) * (1.0 - u)
    other = square * (1.0 - u)
    centre = square * (3.0 - 2.0 * u)
    ahead = c >= 0.0
    below = jnp.where(ahead, -other, 0.0)
    above = jnp.where(ahead, 0.0, other)
    lower = jnp.where(ahead, centre, 0.0)
    upper = jnp.where(ahead, 0.0, -centre)
    a, b = 7.0 / 12.0, 1.0 / 12.0
    return (
        -b * below,
        a * below - b * edge,
        a * (edge + below) - b * above + lower,
        a * (edge + above) - b * below + upper,
        a * above - b * edge,
        -b * above,
    )


def cell_taps(low, high):
    return (
        low[0],
        low[1] - high[0],
        low[2] - high[1],
        1.0 + low[3] - high[2],
        low[4] - high[3],
        low[5] - high[4],
        -high[5],
    )


def transport(
    parity, index, own, up, down, cup, cdown, cf, valid, out, q, c, ends, wx, wy, mid, new, sems
):
    width = own.shape[2]
    ny = own.shape[3]
    group = 24
    strip = HALO * width
    moves = [
        pltpu.make_async_copy(cf.at[parity], c.at[:, pl.ds(4, 8)], sems.at[0]),
        pltpu.make_async_copy(cup.at[pl.ds(strip, 64)], ends.at[0], sems.at[1]),
        pltpu.make_async_copy(cdown.at[pl.ds(strip, 64)], ends.at[1], sems.at[2]),
        pltpu.make_async_copy(up.at[pl.ds(0, strip)], q.at[pl.ds(0, strip)], sems.at[3]),
        pltpu.make_async_copy(down.at[pl.ds(0, strip)], q.at[pl.ds(strip + 8 * width, strip)], sems.at[4]),
    ]
    for row in range(8):
        dst = q.at[pl.ds(strip + row * width, width)]
        moves.append(pltpu.make_async_copy(own.at[row, index], dst, sems.at[5 + row]))
    for move in moves:
        move.start()
    for move in moves[:3]:
        move.wait()
    for d in range(2):
        for row in range(4):
            at = ((d * 2 + parity) * 4 + row) * 4
            for half in (slice(0, 4), slice(4, 8)):
                c[d, row, half, :] = ends[0, at : at + 4, :]
                c[d, row + 12, half, :] = ends[1, at : at + 4, :]
    lane = lax.broadcasted_iota(jnp.int32, (8, ny), 1)
    inside = valid[0, 0]

    def weights(row, carry):
        keep = jnp.where(row < 3, inside, 1.0)
        taps = cell_taps(flux_taps(c[0, row + 1]), flux_taps(c[0, row + 2]))
        for k, w in enumerate(taps):
            wx[row, k] = w * keep
        speed = c[1, row + 1]
        low = flux_taps(speed)
        high = flux_taps(jnp.where(lane == ny - 1, 0.0, pltpu.roll(speed, ny - 1, 1)))
        for k, w in enumerate(cell_taps(low, high)):
            shift = k - 3
            w = jnp.where((lane + shift >= 0) & (lane + shift < ny), w, 0.0)
            wy[row, k] = w
        return carry

    lax.fori_loop(0, 14, weights, 0)
    for move in moves[3:]:
        move.wait()
    parts = range(group // 8)

    def across(values, row):
        w = wy[row, 3]
        totals = [w * v for v in values]
        for shift in (1, 2, 3):
            w = wy[row, 3 + shift]
            totals = [t + w * pltpu.roll(v, ny - shift, 1) for t, v in zip(totals, values)]
            w = wy[row, 3 - shift]
            totals = [t + w * pltpu.roll(v, shift, 1) for t, v in zip(totals, values)]
        return totals

    def along(read, row, base):
        done = [[] for _ in parts]
        for t in range(ny // 128):
            cols = slice(t * 128, t * 128 + 128)
            w = wx[row, 0, :, cols]
            totals = [w * read(base, cols, u) for u in parts]
            for k in range(1, TAPS):
                w = wx[row, k, :, cols]
                totals = [v + w * read(base + k, cols, u) for u, v in enumerate(totals)]
            for u in parts:
                done[u].append(totals[u])
        return [jnp.concatenate(pieces, axis=1) for pieces in done]

    def back(i):
        span = pl.ds(i * group, group)
        return pltpu.make_async_copy(new.at[:, span], out.at[:, 0, span], sems.at[i])

    for i in range(width // group):

        def first(row, cols, u):
            at = pl.multiple_of(row * width + i * group + u * 8, 8)
            return q[pl.ds(at, 8), cols]

        def second(row, cols, u):
            return mid[row, u, :, cols]

        def step_one(row, carry):
            for u, v in enumerate(across(along(first, row, row), row)):
                mid[row, u] = v
            return carry

        def step_two(row, carry):
            for u, v in enumerate(across(along(second, row + 3, row), row + 3)):
                new[row, i * group + u * 8 : i * group + u * 8 + 8, :] = v
            return carry

        lax.fori_loop(0, 14, step_one, 0)
        lax.fori_loop(0, 8, step_two, 0)
        back(i).start()
    for i in range(width // group):
        back(i).wait()


def halves(value):
    top = value.astype(BF16)
    return top, (value - top.astype(F32)).astype(BF16)


def couple(x, matrix, *refs):
    out, wide = refs[-2:]
    species = matrix.shape[0]
    x = x.reshape(species * 4, 128)
    out = out.reshape(species * 4, 128)
    for j in range(4):
        wide[:, j * 128 : j * 128 + 128] = x[pl.ds(j, species, stride=4), :]
    value = wide[...]
    top, rest = halves(value)
    high, low = halves(matrix[...])
    total = jnp.dot(high, top, preferred_element_type=F32)
    total += jnp.dot(high, rest, preferred_element_type=F32)
    total += jnp.dot(low, top, preferred_element_type=F32)
    wide[...] = value + total
    for j in range(4):
        out[pl.ds(j, species, stride=4), :] = wide[:, j * 128 : j * 128 + 128]


def prepare(lm, pbl, land, rates, keep, weven, wodd):
    ny = lm.shape[1]
    kinds = lax.broadcasted_iota(jnp.int32, (rates.shape[1], ny), 0)
    levels = lax.broadcasted_iota(jnp.int32, (8, ny), 0)
    evens = 2 * lax.broadcasted_iota(jnp.int32, (4, ny), 0)
    for r in range(8):
        top = pbl[r : r + 1, :]
        mass = lm[pl.ds(r, 8, stride=8), :]
        total = jnp.sum(jnp.where(levels < top, mass, 0.0), axis=0, keepdims=True)
        scale = 1.0 / total
        even = jnp.where(evens < top, lm[pl.ds(r, 4, stride=16), :], 0.0) * scale
        odd = jnp.where(evens + 1 < top, lm[pl.ds(8 + r, 4, stride=16), :], 0.0) * scale
        weven[r, 0:4, :] = even
        weven[r, 4:8, :] = even
        wodd[r, 0:4, :] = odd
        wodd[r, 4:8, :] = odd
        onehot = (kinds == land[r : r + 1, :]).astype(F32)
        loss = jnp.dot(
            rates[...], onehot, precision=lax.Precision.HIGHEST, preferred_element_type=F32
        )
        keep[r] = jnp.exp(-loss)


def finish(even, odd, keep, weven, wodd, pbl, lm, out, dep, flux):
    ny = even.shape[2]
    sub = lax.broadcasted_iota(jnp.int32, (8, ny), 0)
    level = 2 * (sub % 4)
    first = sub % 2 == 0
    low = sub % 4 < 2
    for r in range(8):
        top = pbl[r : r + 1, :]
        for i in range(even.shape[1] // 8):
            at = slice(i * 8, i * 8 + 8)
            a, b = even[r, at, :], odd[r, at, :]
            total = weven[r] * a + wodd[r] * b
            total += jnp.where(first, pltpu.roll(total, 7, 0), pltpu.roll(total, 1, 0))
            total += jnp.where(low, pltpu.roll(total, 6, 0), pltpu.roll(total, 2, 0))
            a = jnp.where(level < top, total, a)
            b = jnp.where(level + 1 < top, total, b)
            kept = a * keep[r, at, :]
            flux[at, :] = (a - kept) * lm[r : r + 1, :]
            out[pl.ds(i * 128 + r, 8, stride=16), :] = kept
            out[pl.ds(i * 128 + 8 + r, 8, stride=16), :] = b
        count = even.shape[1] // 4
        dep[pl.ds(r, count, stride=8), :] = flux[pl.ds(0, count, stride=4), :]


def on_device(tracers, courant, layer_mass, pbl_top, land_type, rates, coupling):
    own_species, _, rows, ny = tracers.shape
    species = coupling.shape[0]
    width = own_species * 4
    sds = jax.ShapeDtypeStruct
    n_space = lax.axis_size("space")
    up_pairs = [(i, i + 1) for i in range(n_space - 1)]
    down_pairs = [(j, i) for i, j in up_pairs]
    split = tracers.reshape(own_species, 4, 2, rows, ny)
    cf = courant.reshape(-1, ny)
    lm = layer_mass.reshape(-1, ny)
    valid = (lax.axis_index("space") > 0).astype(F32).reshape(1, 1)

    group = sds((rows, width, ny), F32)
    edge = sds((HALO * width + 64, ny), F32)
    speeds = sds((2, 2, rows, 8, ny), F32)
    strips = ny // 128

    def strip(*shape):
        return pl.BlockSpec((*shape, 128), lambda t: (0,) * len(shape) + (t,))

    def level_group(parity):
        shape = (own_species, 4, 1, rows, 128)
        return pl.BlockSpec(shape, lambda t: (0, 0, parity, 0, t))

    even, send_up, send_down, speeds = call(
        pack_even,
        (group, edge, edge, speeds),
        grid=(strips,),
        in_specs=[level_group(0), strip(cf.shape[0])],
        out_specs=[
            strip(rows, width),
            strip(edge.shape[0]),
            strip(edge.shape[0]),
            strip(2, 2, rows, 8),
        ],
    )(split, cf)
    up = lax.ppermute(send_up, "space", up_pairs)
    down = lax.ppermute(send_down, "space", down_pairs)
    odd = call(
        pack_odd,
        group,
        grid=(strips,),
        in_specs=[level_group(1)],
        out_specs=strip(rows, width),
    )(split)

    def exchange(a):
        return lax.all_to_all(a, "spec", split_axis=0, concat_axis=0, tiled=True)

    pair = sds((rows, 2, width, ny), F32)

    def half(index):
        return pl.BlockSpec((rows, 1, width, 128), lambda t: (0, index, 0, t))

    def coupled(a, index, shape, out_index, *into):
        whole = pl.BlockSpec((species, species), lambda t: (0, 0))
        return call(
            couple,
            shape,
            grid=(strips,),
            in_specs=[half(index), whole] + [pl.BlockSpec(memory_space=pl.ANY)] * len(into),
            out_specs=half(out_index),
            scratch_shapes=[pltpu.VMEM((species, 512), F32)],
            input_output_aliases={2: 0} if into else {},
        )(a, coupling, *into)

    cup, cdown = up, down

    def transported(parity, a, index, shape, before, after):
        anywhere = pl.BlockSpec(memory_space=pl.ANY)
        return call(
            functools.partial(transport, parity, index),
            shape,
            in_specs=[anywhere] * 6 + [pl.BlockSpec(memory_space=pltpu.SMEM)],
            out_specs=anywhere,
            scratch_shapes=[
                pltpu.VMEM((20 * width, ny), F32),
                pltpu.VMEM((2, 16, 8, ny), F32),
                pltpu.VMEM((2, 64, ny), F32),
                pltpu.VMEM((14, TAPS, 8, ny), F32),
                pltpu.VMEM((14, TAPS, 8, ny), F32),
                pltpu.VMEM((14, 3, 8, ny), F32),
                pltpu.VMEM((rows, width, ny), F32),
                pltpu.SemaphoreType.DMA((13,)),
            ],
        )(a, before, after, cup, cdown, speeds, valid)

    start = lax.axis_index("spec") * own_species
    mine = lax.dynamic_slice_in_dim(rates, start, own_species, 1).T
    kinds = mine.shape[1]
    mine = jnp.pad(mine[:, None], ((0, 0), (0, 3), (0, 16 - kinds))).reshape(width, 16)
    tile = sds((rows, 8, ny), F32)
    keep, weven, wodd = call(
        prepare,
        (group, tile, tile),
        grid=(strips,),
        in_specs=[
            strip(lm.shape[0]),
            strip(rows),
            strip(rows),
            pl.BlockSpec(mine.shape, lambda t: (0, 0)),
        ],
        out_specs=[strip(rows, width), strip(rows, 8), strip(rows, 8)],
    )(lm, pbl_top, land_type, mine)

    single = sds((rows, 1, width, ny), F32)
    odd = exchange(odd)
    both = transported(0, even[:, None], 0, pair, up, down)
    both = coupled(odd[:, None], 0, pair, 1, both)
    both = exchange(both)
    up = lax.ppermute(both[2:, 1].reshape(-1, ny), "space", up_pairs)
    down = lax.ppermute(both[:HALO, 1].reshape(-1, ny), "space", down_pairs)
    even = coupled(both, 0, single, 0)
    even = exchange(even)[:, 0]
    odd = transported(1, both, 1, single, up, down)[:, 0]

    updated, deposited = call(
        finish,
        (sds((tracers.size // ny, ny), F32), sds((own_species * rows, ny), F32)),
        grid=(strips,),
        in_specs=[strip(rows, width)] * 3 + [strip(rows, 8)] * 2 + [strip(rows)] * 2,
        out_specs=[strip(tracers.size // ny), strip(own_species * rows)],
        scratch_shapes=[pltpu.VMEM((width, 128), F32)],
    )(even, odd, keep, weven, wodd, pbl_top, lm)
    return (updated.reshape(tracers.shape), deposited.reshape(own_species, rows, ny))


def solution(mesh):
    return jax.shard_map(
        on_device,
        mesh=mesh,
        in_specs=(
            P("spec", None, "space", None),
            P(None, None, "space", None),
            P(None, "space", None),
            P("space", None),
            P("space", None),
            P(),
            P(),
        ),
        out_specs=(P("spec", None, "space", None), P("spec", "space", None)),
        check_vma=False,
    )
```

```python
import functools

import jax
import jax.numpy as jnp
from jax import lax
from jax.experimental import pallas as pl
from jax.experimental.pallas import tpu as pltpu
from jax.sharding import PartitionSpec as P


INTERPRET = False
F32 = jnp.float32
BF16 = jnp.bfloat16
TAPS = 7
HALO = 6


def call(body, out_shape, **kw):
    return pl.pallas_call(body, out_shape=out_shape, interpret=INTERPRET, **kw)


def pack_even(x, cf, own, up, down, speeds):
    width = own.shape[2]
    x = x.reshape(width * 8, 128)
    for r in range(8):
        for i in range(width // 8):
            value = x[pl.ds(i * 64 + r, 8, stride=8), :]
            rows = slice(i * 8, i * 8 + 8)
            own[r, 0, rows, :] = value
            if r >= 2:
                up[r - 2, 0, rows, :] = value
            if r < 6:
                down[r, 0, rows, :] = value
    for d in range(2):
        for parity in range(2):
            for row in range(4):
                at = ((d * 2 + parity) * 4 + row) * 4
                start = d * 64 + parity * 8 + row
                before = cf[pl.ds(start, 4, stride=16), :]
                after = cf[pl.ds(start + 4, 4, stride=16), :]
                down[HALO, 0, at : at + 4, :] = before
                up[HALO, 0, at : at + 4, :] = after
                for half in (slice(0, 4), slice(4, 8)):
                    speeds[parity, d, row, half, :] = before
                    speeds[parity, d, row + 4, half, :] = after


def pack_odd(x, own):
    x = x.reshape(own.shape[2] * 8, 128)
    for r in range(8):
        for i in range(own.shape[2] // 8):
            own[r, 0, i * 8 : i * 8 + 8, :] = x[pl.ds(i * 64 + r, 8, stride=8), :]


def flux_taps(c):
    u = jnp.abs(c)
    square = u * u
    edge = c * (1.0 - u) * (1.0 - u)
    other = square * (1.0 - u)
    centre = square * (3.0 - 2.0 * u)
    ahead = c >= 0.0
    below = jnp.where(ahead, -other, 0.0)
    above = jnp.where(ahead, 0.0, other)
    lower = jnp.where(ahead, centre, 0.0)
    upper = jnp.where(ahead, 0.0, -centre)
    a, b = 7.0 / 12.0, 1.0 / 12.0
    return (
        -b * below,
        a * below - b * edge,
        a * (edge + below) - b * above + lower,
        a * (edge + above) - b * below + upper,
        a * above - b * edge,
        -b * above,
    )


def cell_taps(low, high):
    return (
        low[0],
        low[1] - high[0],
        low[2] - high[1],
        1.0 + low[3] - high[2],
        low[4] - high[3],
        low[5] - high[4],
        -high[5],
    )


def transport(
    parity, index, own, up, down, cup, cdown, cf, valid, out, q, c, ends, wx, wy, mid, new, sems
):
    width = own.shape[3]
    strips = own.shape[2]
    ny = strips * 128
    group = 8
    moves = [
        pltpu.make_async_copy(cf.at[parity], c.at[:, pl.ds(4, 8)], sems.at[0]),
        pltpu.make_async_copy(cup.at[HALO, :, pl.ds(0, 64)], ends.at[0], sems.at[1]),
        pltpu.make_async_copy(cdown.at[HALO, :, pl.ds(0, 64)], ends.at[1], sems.at[2]),
        pltpu.make_async_copy(up.at[pl.ds(0, HALO)], q.at[pl.ds(0, HALO)], sems.at[3]),
        pltpu.make_async_copy(own.at[:, index], q.at[pl.ds(HALO, 8)], sems.at[4]),
        pltpu.make_async_copy(down.at[pl.ds(0, HALO)], q.at[pl.ds(HALO + 8, HALO)], sems.at[5]),
    ]
    for move in moves:
        move.start()
    for move in moves[:3]:
        move.wait()
    for d in range(2):
        for row in range(4):
            at = ((d * 2 + parity) * 4 + row) * 4
            for t in range(strips):
                cols = slice(t * 128, t * 128 + 128)
                for half in (slice(0, 4), slice(4, 8)):
                    c[d, row, half, cols] = ends[0, t, at : at + 4, :]
                    c[d, row + 12, half, cols] = ends[1, t, at : at + 4, :]
    lane = lax.broadcasted_iota(jnp.int32, (8, ny), 1)
    inside = valid[0, 0]

    def weights(row, carry):
        keep = jnp.where(row < 3, inside, 1.0)
        taps = cell_taps(flux_taps(c[0, row + 1]), flux_taps(c[0, row + 2]))
        for k, w in enumerate(taps):
            wx[row, k] = w * keep
        speed = c[1, row + 1]
        low = flux_taps(speed)
        high = flux_taps(jnp.where(lane == ny - 1, 0.0, pltpu.roll(speed, ny - 1, 1)))
        for k, w in enumerate(cell_taps(low, high)):
            shift = k - 3
            w = jnp.where((lane + shift >= 0) & (lane + shift < ny), w, 0.0)
            if shift >= 2:
                w = pltpu.roll(w, 3, 1)
            if shift <= -2:
                w = pltpu.roll(w, ny - 3, 1)
            wy[row, k] = w
        return carry

    lax.fori_loop(0, 14, weights, 0)
    for move in moves[3:]:
        move.wait()
    parts = range(group // 8)

    def across(values, row):
        after = [pltpu.roll(v, ny - 1, 1) for v in values]
        before = [pltpu.roll(v, 1, 1) for v in values]
        w = [wy[row, k] for k in range(TAPS)]
        totals = []
        for v, p, m in zip(values, after, before):
            total = w[3] * v + w[4] * p + w[2] * m
            total += pltpu.roll(w[5] * m + w[6] * v, ny - 3, 1)
            total += pltpu.roll(w[1] * p + w[0] * v, 3, 1)
            totals.append(total)
        return totals

    def along(read, row, base):
        done = [[] for _ in parts]
        for t in range(strips):
            cols = slice(t * 128, t * 128 + 128)
            w = wx[row, 0, :, cols]
            totals = [w * read(base, t, u) for u in parts]
            for k in range(1, TAPS):
                w = wx[row, k, :, cols]
                totals = [v + w * read(base + k, t, u) for u, v in enumerate(totals)]
            for u in parts:
                done[u].append(totals[u])
        return [jnp.concatenate(pieces, axis=1) for pieces in done]

    def back(i):
        span = pl.ds(pl.multiple_of(i * group, 8), group)
        return pltpu.make_async_copy(new.at[:, :, span], out.at[:, 0, :, span], sems.at[i])

    def block(i, carry):
        places = [pl.multiple_of(i * group + u * 8, 8) for u in parts]

        def first(row, t, u):
            return q[row, t, pl.ds(places[u], 8), :]

        def second(row, t, u):
            return mid[row, u, :, t * 128 : t * 128 + 128]

        for row in range(14):
            for u, v in enumerate(across(along(first, row, row), row)):
                mid[row, u] = v
            late = row - 6
            if late >= 0:
                for u, v in enumerate(across(along(second, late + 3, late), late + 3)):
                    for t in range(strips):
                        new[late, t, pl.ds(places[u], 8), :] = v[:, t * 128 : t * 128 + 128]
        back(i).start()
        return carry

    lax.fori_loop(0, width // group, block, 0)
    for i in range(width // group):
        back(i).wait()


def halves(value):
    top = value.astype(BF16)
    return top, (value - top.astype(F32)).astype(BF16)


def couple(x, matrix, *refs):
    out, wide = refs[-2:]
    species = matrix.shape[0]
    x = x.reshape(species * 4, 128)
    out = out.reshape(species * 4, 128)
    for j in range(4):
        wide[:, j * 128 : j * 128 + 128] = x[pl.ds(j, species, stride=4), :]
    value = wide[...]
    top, rest = halves(value)
    high, low = halves(matrix[...])
    total = jnp.dot(high, top, preferred_element_type=F32)
    total += jnp.dot(high, rest, preferred_element_type=F32)
    total += jnp.dot(low, top, preferred_element_type=F32)
    wide[...] = value + total
    for j in range(4):
        out[pl.ds(j, species, stride=4), :] = wide[:, j * 128 : j * 128 + 128]


def prepare(lm, pbl, land, rates, keep, weven, wodd):
    ny = lm.shape[1]
    kinds = lax.broadcasted_iota(jnp.int32, (rates.shape[1], ny), 0)
    levels = lax.broadcasted_iota(jnp.int32, (8, ny), 0)
    evens = 2 * lax.broadcasted_iota(jnp.int32, (4, ny), 0)
    for r in range(8):
        top = pbl[r : r + 1, :]
        mass = lm[pl.ds(r, 8, stride=8), :]
        total = jnp.sum(jnp.where(levels < top, mass, 0.0), axis=0, keepdims=True)
        scale = 1.0 / total
        even = jnp.where(evens < top, lm[pl.ds(r, 4, stride=16), :], 0.0) * scale
        odd = jnp.where(evens + 1 < top, lm[pl.ds(8 + r, 4, stride=16), :], 0.0) * scale
        weven[r, 0:4, :] = even
        weven[r, 4:8, :] = even
        wodd[r, 0:4, :] = odd
        wodd[r, 4:8, :] = odd
        onehot = (kinds == land[r : r + 1, :]).astype(F32)
        loss = jnp.dot(
            rates[...], onehot, precision=lax.Precision.HIGHEST, preferred_element_type=F32
        )
        keep[r, 0] = jnp.exp(-loss)


def finish(even, odd, keep, weven, wodd, pbl, lm, out, dep, flux):
    ny = even.shape[3]
    width = even.shape[2]
    sub = lax.broadcasted_iota(jnp.int32, (8, ny), 0)
    level = 2 * (sub % 4)
    first = sub % 2 == 0
    low = sub % 4 < 2
    for r in range(8):
        top = pbl[r : r + 1, :]
        for i in range(width // 8):
            at = slice(i * 8, i * 8 + 8)
            a, b = even[r, 0, at, :], odd[r, 0, at, :]
            total = weven[r] * a + wodd[r] * b
            total += jnp.where(first, pltpu.roll(total, 7, 0), pltpu.roll(total, 1, 0))
            total += jnp.where(low, pltpu.roll(total, 6, 0), pltpu.roll(total, 2, 0))
            a = jnp.where(level < top, total, a)
            b = jnp.where(level + 1 < top, total, b)
            kept = a * keep[r, 0, at, :]
            flux[at, :] = (a - kept) * lm[r : r + 1, :]
            out[pl.ds(i * 128 + r, 8, stride=16), :] = kept
            out[pl.ds(i * 128 + 8 + r, 8, stride=16), :] = b
        count = width // 4
        dep[pl.ds(r, count, stride=8), :] = flux[pl.ds(0, count, stride=4), :]


def on_device(tracers, courant, layer_mass, pbl_top, land_type, rates, coupling):
    own_species, _, rows, ny = tracers.shape
    species = coupling.shape[0]
    width = own_species * 4
    sds = jax.ShapeDtypeStruct
    n_space = lax.axis_size("space")
    up_pairs = [(i, i + 1) for i in range(n_space - 1)]
    down_pairs = [(j, i) for i, j in up_pairs]
    split = tracers.reshape(own_species, 4, 2, rows, ny)
    cf = courant.reshape(-1, ny)
    lm = layer_mass.reshape(-1, ny)
    valid = (lax.axis_index("space") > 0).astype(F32).reshape(1, 1)

    strips = ny // 128
    group = sds((rows, strips, width, 128), F32)
    edge = sds((HALO + 1, strips, width, 128), F32)
    speeds = sds((2, 2, rows, 8, ny), F32)

    def strip(*shape):
        return pl.BlockSpec((*shape, 128), lambda t: (0,) * len(shape) + (t,))

    def columns(count):
        return pl.BlockSpec((count, 1, width, 128), lambda t: (0, t, 0, 0))

    def level_group(parity):
        shape = (own_species, 4, 1, rows, 128)
        return pl.BlockSpec(shape, lambda t: (0, 0, parity, 0, t))

    even, send_up, send_down, speeds = call(
        pack_even,
        (group, edge, edge, speeds),
        grid=(strips,),
        in_specs=[level_group(0), strip(cf.shape[0])],
        out_specs=[
            columns(rows),
            columns(HALO + 1),
            columns(HALO + 1),
            strip(2, 2, rows, 8),
        ],
    )(split, cf)
    up = lax.ppermute(send_up, "space", up_pairs)
    down = lax.ppermute(send_down, "space", down_pairs)
    odd = call(
        pack_odd,
        group,
        grid=(strips,),
        in_specs=[level_group(1)],
        out_specs=columns(rows),
    )(split)

    def exchange(a):
        return lax.all_to_all(a, "spec", split_axis=0, concat_axis=0, tiled=True)

    pair = sds((rows, 2, strips, width, 128), F32)

    def half(index):
        return pl.BlockSpec((rows, 1, 1, width, 128), lambda t: (0, index, t, 0, 0))

    def coupled(a, index, shape, out_index, *into):
        whole = pl.BlockSpec((species, species), lambda t: (0, 0))
        return call(
            couple,
            shape,
            grid=(strips,),
            in_specs=[half(index), whole] + [pl.BlockSpec(memory_space=pl.ANY)] * len(into),
            out_specs=half(out_index),
            scratch_shapes=[pltpu.VMEM((species, 512), F32)],
            input_output_aliases={2: 0} if into else {},
        )(a, coupling, *into)

    cup, cdown = up, down

    def transported(parity, a, index, shape, before, after):
        anywhere = pl.BlockSpec(memory_space=pl.ANY)
        return call(
            functools.partial(transport, parity, index),
            shape,
            in_specs=[anywhere] * 6 + [pl.BlockSpec(memory_space=pltpu.SMEM)],
            out_specs=anywhere,
            scratch_shapes=[
                pltpu.VMEM((20, strips, width, 128), F32),
                pltpu.VMEM((2, 16, 8, ny), F32),
                pltpu.VMEM((2, strips, 64, 128), F32),
                pltpu.VMEM((14, TAPS, 8, ny), F32),
                pltpu.VMEM((14, TAPS, 8, ny), F32),
                pltpu.VMEM((14, 1, 8, ny), F32),
                pltpu.VMEM((rows, strips, width, 128), F32),
                pltpu.SemaphoreType.DMA((15,)),
            ],
        )(a, before, after, cup, cdown, speeds, valid)

    start = lax.axis_index("spec") * own_species
    mine = lax.dynamic_slice_in_dim(rates, start, own_species, 1).T
    kinds = mine.shape[1]
    mine = jnp.pad(mine[:, None], ((0, 0), (0, 3), (0, 16 - kinds))).reshape(width, 16)
    tile = sds((rows, 8, ny), F32)
    keep, weven, wodd = call(
        prepare,
        (group, tile, tile),
        grid=(strips,),
        in_specs=[
            strip(lm.shape[0]),
            strip(rows),
            strip(rows),
            pl.BlockSpec(mine.shape, lambda t: (0, 0)),
        ],
        out_specs=[columns(rows), strip(rows, 8), strip(rows, 8)],
    )(lm, pbl_top, land_type, mine)

    single = sds((rows, 1, strips, width, 128), F32)
    odd = exchange(odd)
    both = transported(0, even[:, None], 0, pair, up, down)
    both = coupled(odd[:, None], 0, pair, 1, both)
    both = exchange(both)
    up = lax.ppermute(both[2:, 1], "space", up_pairs)
    down = lax.ppermute(both[:HALO, 1], "space", down_pairs)
    even = coupled(both, 0, single, 0)
    even = exchange(even)[:, 0]
    odd = transported(1, both, 1, single, up, down)[:, 0]

    updated, deposited = call(
        finish,
        (sds((tracers.size // ny, ny), F32), sds((own_species * rows, ny), F32)),
        grid=(strips,),
        in_specs=[columns(rows)] * 3 + [strip(rows, 8)] * 2 + [strip(rows)] * 2,
        out_specs=[strip(tracers.size // ny), strip(own_species * rows)],
        scratch_shapes=[pltpu.VMEM((width, 128), F32)],
    )(even, odd, keep, weven, wodd, pbl_top, lm)
    return (updated.reshape(tracers.shape), deposited.reshape(own_species, rows, ny))


def solution(mesh):
    return jax.shard_map(
        on_device,
        mesh=mesh,
        in_specs=(
            P("spec", None, "space", None),
            P(None, None, "space", None),
            P(None, "space", None),
            P("space", None),
            P("space", None),
            P(),
            P(),
        ),
        out_specs=(P("spec", None, "space", None), P("spec", "space", None)),
        check_vma=False,
    )
```

```python
import functools

import jax
import jax.numpy as jnp
from jax import lax
from jax.experimental import pallas as pl
from jax.experimental.pallas import tpu as pltpu
from jax.sharding import PartitionSpec as P


INTERPRET = False
F32 = jnp.float32
BF16 = jnp.bfloat16
TAPS = 7
GRANT = 48 << 20
HALO = 6


def near(array):
    return array if INTERPRET else pltpu.with_memory_space_constraint(array, pltpu.VMEM)


def far(array):
    return array if INTERPRET else pltpu.with_memory_space_constraint(array, pltpu.HBM)


def far_shape(shape):
    return jax.ShapeDtypeStruct(shape, F32) if INTERPRET else pltpu.HBM(shape, F32)


def call(body, out_shape, grant=None, **kw):
    params = pltpu.CompilerParams(vmem_limit_bytes=grant)
    return pl.pallas_call(
        body, out_shape=out_shape, interpret=INTERPRET, compiler_params=params, **kw
    )


def pack_even(x, cf, own, up, down, speeds):
    width = own.shape[2]
    x = x.reshape(width * 8, 128)
    for r in range(8):
        for i in range(width // 8):
            value = x[pl.ds(i * 64 + r, 8, stride=8), :]
            rows = slice(i * 8, i * 8 + 8)
            own[r, 0, rows, :] = value
            if r >= 2:
                up[r - 2, 0, rows, :] = value
            if r < 6:
                down[r, 0, rows, :] = value
    for d in range(2):
        for parity in range(2):
            for row in range(4):
                at = ((d * 2 + parity) * 4 + row) * 4
                start = d * 64 + parity * 8 + row
                before = cf[pl.ds(start, 4, stride=16), :]
                after = cf[pl.ds(start + 4, 4, stride=16), :]
                down[HALO, 0, at : at + 4, :] = before
                up[HALO, 0, at : at + 4, :] = after
                for half in (slice(0, 4), slice(4, 8)):
                    speeds[parity, d, row, half, :] = before
                    speeds[parity, d, row + 4, half, :] = after


def pack_odd(x, own):
    x = x.reshape(own.shape[2] * 8, 128)
    for r in range(8):
        for i in range(own.shape[2] // 8):
            own[r, 0, i * 8 : i * 8 + 8, :] = x[pl.ds(i * 64 + r, 8, stride=8), :]


def flux_taps(c):
    u = jnp.abs(c)
    square = u * u
    edge = c * (1.0 - u) * (1.0 - u)
    other = square * (1.0 - u)
    centre = square * (3.0 - 2.0 * u)
    ahead = c >= 0.0
    below = jnp.where(ahead, -other, 0.0)
    above = jnp.where(ahead, 0.0, other)
    lower = jnp.where(ahead, centre, 0.0)
    upper = jnp.where(ahead, 0.0, -centre)
    a, b = 7.0 / 12.0, 1.0 / 12.0
    return (
        -b * below,
        a * below - b * edge,
        a * (edge + below) - b * above + lower,
        a * (edge + above) - b * below + upper,
        a * above - b * edge,
        -b * above,
    )


def cell_taps(low, high):
    return (
        low[0],
        low[1] - high[0],
        low[2] - high[1],
        1.0 + low[3] - high[2],
        low[4] - high[3],
        low[5] - high[4],
        -high[5],
    )


def transport(
    parity, index, own, up, down, cup, cdown, cf, valid, out, q, c, ends, wx, wy, mid, new, sems
):
    width = own.shape[3]
    strips = own.shape[2]
    ny = strips * 128
    group = 8
    moves = [
        pltpu.make_async_copy(cf.at[parity], c.at[:, pl.ds(4, 8)], sems.at[0]),
        pltpu.make_async_copy(cup.at[HALO, :, pl.ds(0, 64)], ends.at[0], sems.at[1]),
        pltpu.make_async_copy(cdown.at[HALO, :, pl.ds(0, 64)], ends.at[1], sems.at[2]),
        pltpu.make_async_copy(up.at[pl.ds(0, HALO)], q.at[pl.ds(0, HALO)], sems.at[3]),
        pltpu.make_async_copy(own.at[:, index], q.at[pl.ds(HALO, 8)], sems.at[4]),
        pltpu.make_async_copy(down.at[pl.ds(0, HALO)], q.at[pl.ds(HALO + 8, HALO)], sems.at[5]),
    ]
    for move in moves:
        move.start()
    for move in moves[:3]:
        move.wait()
    for d in range(2):
        for row in range(4):
            at = ((d * 2 + parity) * 4 + row) * 4
            for t in range(strips):
                cols = slice(t * 128, t * 128 + 128)
                for half in (slice(0, 4), slice(4, 8)):
                    c[d, row, half, cols] = ends[0, t, at : at + 4, :]
                    c[d, row + 12, half, cols] = ends[1, t, at : at + 4, :]
    lane = lax.broadcasted_iota(jnp.int32, (8, ny), 1)
    inside = valid[0, 0]

    def weights(row, carry):
        keep = jnp.where(row < 3, inside, 1.0)
        taps = cell_taps(flux_taps(c[0, row + 1]), flux_taps(c[0, row + 2]))
        for k, w in enumerate(taps):
            wx[row, k] = w * keep
        speed = c[1, row + 1]
        low = flux_taps(speed)
        high = flux_taps(jnp.where(lane == ny - 1, 0.0, pltpu.roll(speed, ny - 1, 1)))
        for k, w in enumerate(cell_taps(low, high)):
            shift = k - 3
            w = jnp.where((lane + shift >= 0) & (lane + shift < ny), w, 0.0)
            if shift >= 2:
                w = pltpu.roll(w, 3, 1)
            if shift <= -2:
                w = pltpu.roll(w, ny - 3, 1)
            wy[row, k] = w
        return carry

    lax.fori_loop(0, 14, weights, 0)
    for move in moves[3:]:
        move.wait()
    parts = range(group // 8)

    def across(values, row):
        after = [pltpu.roll(v, ny - 1, 1) for v in values]
        before = [pltpu.roll(v, 1, 1) for v in values]
        w = [wy[row, k] for k in range(TAPS)]
        totals = []
        for v, p, m in zip(values, after, before):
            total = w[3] * v + w[4] * p + w[2] * m
            total += pltpu.roll(w[5] * m + w[6] * v, ny - 3, 1)
            total += pltpu.roll(w[1] * p + w[0] * v, 3, 1)
            totals.append(total)
        return totals

    def along(read, row, base):
        done = [[] for _ in parts]
        for t in range(strips):
            cols = slice(t * 128, t * 128 + 128)
            w = wx[row, 0, :, cols]
            totals = [w * read(base, t, u) for u in parts]
            for k in range(1, TAPS):
                w = wx[row, k, :, cols]
                totals = [v + w * read(base + k, t, u) for u, v in enumerate(totals)]
            for u in parts:
                done[u].append(totals[u])
        return [jnp.concatenate(pieces, axis=1) for pieces in done]

    def back(i):
        span = pl.ds(pl.multiple_of(i * group, 8), group)
        return pltpu.make_async_copy(new.at[:, :, span], out.at[:, 0, :, span], sems.at[i])

    def block(i, carry):
        places = [pl.multiple_of(i * group + u * 8, 8) for u in parts]

        def first(row, t, u):
            return q[row, t, pl.ds(places[u], 8), :]

        def second(row, t, u):
            return mid[row, u, :, t * 128 : t * 128 + 128]

        for row in range(14):
            for u, v in enumerate(across(along(first, row, row), row)):
                mid[row, u] = v
            late = row - 6
            if late >= 0:
                for u, v in enumerate(across(along(second, late + 3, late), late + 3)):
                    for t in range(strips):
                        new[late, t, pl.ds(places[u], 8), :] = v[:, t * 128 : t * 128 + 128]
        back(i).start()
        return carry

    lax.fori_loop(0, width // group, block, 0)
    for i in range(width // group):
        back(i).wait()


def halves(value):
    top = value.astype(BF16)
    return top, (value - top.astype(F32)).astype(BF16)


def couple(index, place, x, matrix, *refs):
    out, wide, line, come, go = refs[-5:]
    species = matrix.shape[0]
    rows, strips, width = x.shape[0], x.shape[2], x.shape[3]

    def part(t, d):
        return line.at[t, pl.ds(d * width, width)]

    blocks = [(t, d) for t in range(strips) for d in range(rows)]
    inward = {k: pltpu.make_async_copy(x.at[k[1], index, k[0]], part(*k), come.at[*k]) for k in blocks}
    outward = {k: pltpu.make_async_copy(part(*k), out.at[k[1], place, k[0]], go.at[*k]) for k in blocks}
    for k in blocks:
        inward[k].start()
    high, low = halves(matrix[...])
    for t in range(strips):
        for d in range(rows):
            inward[t, d].wait()
        for j in range(4):
            wide[:, j * 128 : j * 128 + 128] = line.at[t][pl.ds(j, species, stride=4), :]
        value = wide[...]
        top, rest = halves(value)
        total = jnp.dot(high, top, preferred_element_type=F32)
        total += jnp.dot(high, rest, preferred_element_type=F32)
        total += jnp.dot(low, top, preferred_element_type=F32)
        wide[...] = value + total
        for j in range(4):
            line.at[t][pl.ds(j, species, stride=4), :] = wide[:, j * 128 : j * 128 + 128]
        for d in range(rows):
            outward[t, d].start()
    for k in blocks:
        outward[k].wait()


def prepare(lm, pbl, land, rates, keep, weven, wodd):
    ny = lm.shape[1]
    kinds = lax.broadcasted_iota(jnp.int32, (rates.shape[1], ny), 0)
    levels = lax.broadcasted_iota(jnp.int32, (8, ny), 0)
    evens = 2 * lax.broadcasted_iota(jnp.int32, (4, ny), 0)
    for r in range(8):
        top = pbl[r : r + 1, :]
        mass = lm[pl.ds(r, 8, stride=8), :]
        total = jnp.sum(jnp.where(levels < top, mass, 0.0), axis=0, keepdims=True)
        scale = 1.0 / total
        even = jnp.where(evens < top, lm[pl.ds(r, 4, stride=16), :], 0.0) * scale
        odd = jnp.where(evens + 1 < top, lm[pl.ds(8 + r, 4, stride=16), :], 0.0) * scale
        weven[r, 0:4, :] = even
        weven[r, 4:8, :] = even
        wodd[r, 0:4, :] = odd
        wodd[r, 4:8, :] = odd
        onehot = (kinds == land[r : r + 1, :]).astype(F32)
        loss = jnp.dot(
            rates[...], onehot, precision=lax.Precision.HIGHEST, preferred_element_type=F32
        )
        keep[r, 0] = jnp.exp(-loss)


def finish(even, odd, keep, weven, wodd, pbl, lm, out, dep, flux):
    t = pl.program_id(0)
    ny = even.shape[3]
    width = even.shape[2]
    sub = lax.broadcasted_iota(jnp.int32, (8, ny), 0)
    level = 2 * (sub % 4)
    first = sub % 2 == 0
    low = sub % 4 < 2
    for r in range(8):
        top = pbl[r : r + 1, :]
        for i in range(width // 8):
            at = slice(i * 8, i * 8 + 8)
            a, b = even[r, t, at, :], odd[r, 0, at, :]
            total = weven[r] * a + wodd[r] * b
            total += jnp.where(first, pltpu.roll(total, 7, 0), pltpu.roll(total, 1, 0))
            total += jnp.where(low, pltpu.roll(total, 6, 0), pltpu.roll(total, 2, 0))
            a = jnp.where(level < top, total, a)
            b = jnp.where(level + 1 < top, total, b)
            kept = a * keep[r, 0, at, :]
            flux[at, :] = (a - kept) * lm[r : r + 1, :]
            out[pl.ds(i * 128 + r, 8, stride=16), :] = kept
            out[pl.ds(i * 128 + 8 + r, 8, stride=16), :] = b
        count = width // 4
        dep[pl.ds(r, count, stride=8), :] = flux[pl.ds(0, count, stride=4), :]


def on_device(tracers, courant, layer_mass, pbl_top, land_type, rates, coupling):
    own_species, _, rows, ny = tracers.shape
    species = coupling.shape[0]
    width = own_species * 4
    sds = jax.ShapeDtypeStruct
    n_space = lax.axis_size("space")
    up_pairs = [(i, i + 1) for i in range(n_space - 1)]
    down_pairs = [(j, i) for i, j in up_pairs]
    split = tracers.reshape(own_species, 4, 2, rows, ny)
    cf = courant.reshape(-1, ny)
    lm = layer_mass.reshape(-1, ny)
    valid = (lax.axis_index("space") > 0).astype(F32).reshape(1, 1)

    strips = ny // 128
    group = sds((rows, strips, width, 128), F32)
    edge = sds((HALO + 1, strips, width, 128), F32)
    speeds = sds((2, 2, rows, 8, ny), F32)

    def strip(*shape):
        return pl.BlockSpec((*shape, 128), lambda t: (0,) * len(shape) + (t,))

    def columns(count):
        return pl.BlockSpec((count, 1, width, 128), lambda t: (0, t, 0, 0))

    def level_group(parity):
        shape = (own_species, 4, 1, rows, 128)
        return pl.BlockSpec(shape, lambda t: (0, 0, parity, 0, t))

    even, send_up, send_down, speeds = call(
        pack_even,
        (group, edge, edge, speeds),
        grid=(strips,),
        in_specs=[level_group(0), strip(cf.shape[0])],
        out_specs=[
            columns(rows),
            columns(HALO + 1),
            columns(HALO + 1),
            strip(2, 2, rows, 8),
        ],
    )(split, cf)
    up = lax.ppermute(send_up, "space", up_pairs)
    down = lax.ppermute(send_down, "space", down_pairs)
    odd = call(
        pack_odd,
        group,
        grid=(strips,),
        in_specs=[level_group(1)],
        out_specs=columns(rows),
    )(split)

    def exchange(a):
        return lax.all_to_all(a, "spec", split_axis=0, concat_axis=0, tiled=True)

    pair = far_shape((rows, 2, strips, width, 128))

    whole = pl.BlockSpec(memory_space=pltpu.VMEM)
    anywhere = pl.BlockSpec(memory_space=pl.ANY)
    far_spec = anywhere if INTERPRET else pl.BlockSpec(memory_space=pltpu.HBM)

    def coupled(a, index, shape, place, *into):
        return call(
            functools.partial(couple, index, place),
            shape,
            in_specs=[anywhere, whole] + [far_spec] * len(into),
            out_specs=far_spec,
            scratch_shapes=[
                pltpu.VMEM((species, 512), F32),
                pltpu.VMEM((strips, species * 4, 128), F32),
                pltpu.SemaphoreType.DMA((strips, rows)),
                pltpu.SemaphoreType.DMA((strips, rows)),
            ],
            input_output_aliases={2: 0} if into else {},
        )(a, coupling, *into)

    cup, cdown = up, down

    def transported(parity, a, index, shape, before, after):
        return call(
            functools.partial(transport, parity, index),
            shape,
            grant=GRANT,
            in_specs=[anywhere] * 6 + [pl.BlockSpec(memory_space=pltpu.SMEM)],
            out_specs=far_spec,
            scratch_shapes=[
                pltpu.VMEM((20, strips, width, 128), F32),
                pltpu.VMEM((2, 16, 8, ny), F32),
                pltpu.VMEM((2, strips, 64, 128), F32),
                pltpu.VMEM((14, TAPS, 8, ny), F32),
                pltpu.VMEM((14, TAPS, 8, ny), F32),
                pltpu.VMEM((14, 1, 8, ny), F32),
                pltpu.VMEM((rows, strips, width, 128), F32),
                pltpu.SemaphoreType.DMA((15,)),
            ],
        )(far(a) if index == 0 else a, before, after, cup, cdown, far(speeds), valid)

    start = lax.axis_index("spec") * own_species
    mine = lax.dynamic_slice_in_dim(rates, start, own_species, 1).T
    kinds = mine.shape[1]
    mine = jnp.pad(mine[:, None], ((0, 0), (0, 3), (0, 16 - kinds))).reshape(width, 16)
    tile = sds((rows, 8, ny), F32)
    keep, weven, wodd = call(
        prepare,
        (group, tile, tile),
        grid=(strips,),
        in_specs=[
            strip(lm.shape[0]),
            strip(rows),
            strip(rows),
            pl.BlockSpec(mine.shape, lambda t: (0, 0)),
        ],
        out_specs=[columns(rows), strip(rows, 8), strip(rows, 8)],
    )(lm, pbl_top, land_type, mine)

    single = far_shape((rows, 1, strips, width, 128))
    odd = exchange(odd)
    both = transported(0, even[:, None], 0, pair, up, down)
    both = coupled(odd[:, None], 0, pair, 1, both)
    both = exchange(both)
    up = lax.ppermute(both[2:, 1], "space", up_pairs)
    down = lax.ppermute(both[:HALO, 1], "space", down_pairs)
    even = coupled(both, 0, single, 0)
    even = exchange(even)[:, 0]
    odd = transported(1, both, 1, single, up, down)[:, 0]

    updated, deposited = call(
        finish,
        (sds((tracers.size // ny, ny), F32), sds((own_species * rows, ny), F32)),
        grid=(strips,),
        in_specs=[whole] + [columns(rows)] * 2 + [strip(rows, 8)] * 2 + [strip(rows)] * 2,
        out_specs=[strip(tracers.size // ny), strip(own_species * rows)],
        scratch_shapes=[pltpu.VMEM((width, 128), F32)],
    )(near(even), odd, keep, weven, wodd, pbl_top, lm)
    return (updated.reshape(tracers.shape), deposited.reshape(own_species, rows, ny))


def solution(mesh):
    return jax.shard_map(
        on_device,
        mesh=mesh,
        in_specs=(
            P("spec", None, "space", None),
            P(None, None, "space", None),
            P(None, "space", None),
            P("space", None),
            P("space", None),
            P(),
            P(),
        ),
        out_specs=(P("spec", None, "space", None), P("spec", "space", None)),
        check_vma=False,
    )
```

```python
import functools

import jax
import jax.numpy as jnp
from jax import lax
from jax.experimental import pallas as pl
from jax.experimental.pallas import tpu as pltpu
from jax.sharding import PartitionSpec as P


INTERPRET = False
F32 = jnp.float32
BF16 = jnp.bfloat16
TAPS = 7
GRANT = 48 << 20
HALO = 6


def near(array):
    return array if INTERPRET else pltpu.with_memory_space_constraint(array, pltpu.VMEM)


def far(array):
    return array if INTERPRET else pltpu.with_memory_space_constraint(array, pltpu.HBM)


def far_shape(shape):
    return jax.ShapeDtypeStruct(shape, F32) if INTERPRET else pltpu.HBM(shape, F32)


def call(body, out_shape, grant=None, **kw):
    params = pltpu.CompilerParams(vmem_limit_bytes=grant)
    return pl.pallas_call(
        body, out_shape=out_shape, interpret=INTERPRET, compiler_params=params, **kw
    )


def pack_even(x, cf, own, up, down, speeds):
    width = own.shape[2]
    x = x.reshape(width * 8, 128)
    for r in range(8):
        for i in range(width // 8):
            value = x[pl.ds(i * 64 + r, 8, stride=8), :]
            rows = slice(i * 8, i * 8 + 8)
            own[r, 0, rows, :] = value
            if r >= 2:
                at = (r - 2) * width + i * 8
                up[0, at : at + 8, :] = value
            if r < 6:
                at = r * width + i * 8
                down[0, at : at + 8, :] = value
    for d in range(2):
        for parity in range(2):
            for row in range(4):
                at = HALO * width + ((d * 2 + parity) * 4 + row) * 4
                start = d * 64 + parity * 8 + row
                before = cf[pl.ds(start, 4, stride=16), :]
                after = cf[pl.ds(start + 4, 4, stride=16), :]
                down[0, at : at + 4, :] = before
                up[0, at : at + 4, :] = after
                for half in (slice(0, 4), slice(4, 8)):
                    speeds[parity, d, row, half, :] = before
                    speeds[parity, d, row + 4, half, :] = after


def pack_odd(x, own):
    x = x.reshape(own.shape[2] * 8, 128)
    for r in range(8):
        for i in range(own.shape[2] // 8):
            own[r, 0, i * 8 : i * 8 + 8, :] = x[pl.ds(i * 64 + r, 8, stride=8), :]


def flux_taps(c):
    u = jnp.abs(c)
    square = u * u
    edge = c * (1.0 - u) * (1.0 - u)
    other = square * (1.0 - u)
    centre = square * (3.0 - 2.0 * u)
    ahead = c >= 0.0
    below = jnp.where(ahead, -other, 0.0)
    above = jnp.where(ahead, 0.0, other)
    lower = jnp.where(ahead, centre, 0.0)
    upper = jnp.where(ahead, 0.0, -centre)
    a, b = 7.0 / 12.0, 1.0 / 12.0
    return (
        -b * below,
        a * below - b * edge,
        a * (edge + below) - b * above + lower,
        a * (edge + above) - b * below + upper,
        a * above - b * edge,
        -b * above,
    )


def cell_taps(low, high):
    return (
        low[0],
        low[1] - high[0],
        low[2] - high[1],
        1.0 + low[3] - high[2],
        low[4] - high[3],
        low[5] - high[4],
        -high[5],
    )


def transport(
    parity, index, own, up, down, cup, cdown, cf, valid, out, q, c, ends, wx, wy, mid, new, sems
):
    width = own.shape[3]
    strips = own.shape[2]
    ny = strips * 128
    group = 24
    tail = pl.ds(HALO * width, 64)
    moves = [
        pltpu.make_async_copy(cf.at[parity], c.at[:, pl.ds(4, 8)], sems.at[0]),
        pltpu.make_async_copy(cup.at[:, tail], ends.at[0], sems.at[1]),
        pltpu.make_async_copy(cdown.at[:, tail], ends.at[1], sems.at[2]),
        pltpu.make_async_copy(own.at[:, index], q.at[pl.ds(HALO, 8)], sems.at[3]),
    ]
    for row in range(HALO):
        span = pl.ds(row * width, width)
        before = up.at[:, span] if index == 0 else up.at[row]
        after = down.at[:, span] if index == 0 else down.at[row]
        moves.append(pltpu.make_async_copy(before, q.at[row], sems.at[4 + row]))
        moves.append(pltpu.make_async_copy(after, q.at[HALO + 8 + row], sems.at[10 + row]))
    for move in moves:
        move.start()
    for move in moves[:3]:
        move.wait()
    for d in range(2):
        for row in range(4):
            at = ((d * 2 + parity) * 4 + row) * 4
            for t in range(strips):
                cols = slice(t * 128, t * 128 + 128)
                for half in (slice(0, 4), slice(4, 8)):
                    c[d, row, half, cols] = ends[0, t, at : at + 4, :]
                    c[d, row + 12, half, cols] = ends[1, t, at : at + 4, :]
    lane = lax.broadcasted_iota(jnp.int32, (8, ny), 1)
    inside = valid[0, 0]

    def weights(row, carry):
        keep = jnp.where(row < 3, inside, 1.0)
        taps = cell_taps(flux_taps(c[0, row + 1]), flux_taps(c[0, row + 2]))
        for k, w in enumerate(taps):
            wx[row, k] = w * keep
        speed = c[1, row + 1]
        low = flux_taps(speed)
        high = flux_taps(jnp.where(lane == ny - 1, 0.0, pltpu.roll(speed, ny - 1, 1)))
        for k, w in enumerate(cell_taps(low, high)):
            shift = k - 3
            w = jnp.where((lane + shift >= 0) & (lane + shift < ny), w, 0.0)
            wy[row, k] = w
        return carry

    lax.fori_loop(0, 14, weights, 0)
    for move in moves[3:]:
        move.wait()
    parts = range(group // 8)

    def across(values, row):
        w = wy[row, 3]
        totals = [w * v for v in values]
        for shift in (1, 2, 3):
            w = wy[row, 3 + shift]
            totals = [t + w * pltpu.roll(v, ny - shift, 1) for t, v in zip(totals, values)]
            w = wy[row, 3 - shift]
            totals = [t + w * pltpu.roll(v, shift, 1) for t, v in zip(totals, values)]
        return totals

    def along(read, row, base):
        done = [[] for _ in parts]
        for t in range(strips):
            cols = slice(t * 128, t * 128 + 128)
            w = wx[row, 0, :, cols]
            totals = [w * read(base, t, u) for u in parts]
            for k in range(1, TAPS):
                w = wx[row, k, :, cols]
                totals = [v + w * read(base + k, t, u) for u, v in enumerate(totals)]
            for u in parts:
                done[u].append(totals[u])
        return [jnp.concatenate(pieces, axis=1) for pieces in done]

    def back(i):
        span = pl.ds(pl.multiple_of(i * group, 8), group)
        return pltpu.make_async_copy(new.at[:, :, span], out.at[:, 0, :, span], sems.at[i])

    def block(i, carry):
        places = [pl.multiple_of(i * group + u * 8, 8) for u in parts]

        def first(row, t, u):
            return q[row, t, pl.ds(places[u], 8), :]

        def second(row, t, u):
            return mid[row, u, :, t * 128 : t * 128 + 128]

        for row in range(14):
            for u, v in enumerate(across(along(first, row, row), row)):
                mid[row, u] = v
        for row in range(8):
            for u, v in enumerate(across(along(second, row + 3, row), row + 3)):
                for t in range(strips):
                    new[row, t, pl.ds(places[u], 8), :] = v[:, t * 128 : t * 128 + 128]
        back(i).start()
        return carry

    lax.fori_loop(0, width // group, block, 0)
    for i in range(width // group):
        back(i).wait()


def halves(value):
    top = value.astype(BF16)
    return top, (value - top.astype(F32)).astype(BF16)


def couple(index, place, x, matrix, *refs):
    out, wide, line, come, go = refs[-5:]
    species = matrix.shape[0]
    rows, strips, width = x.shape[0], x.shape[2], x.shape[3]

    def part(t, d):
        return line.at[t, pl.ds(d * width, width)]

    blocks = [(t, d) for t in range(strips) for d in range(rows)]
    inward = {k: pltpu.make_async_copy(x.at[k[1], index, k[0]], part(*k), come.at[*k]) for k in blocks}
    outward = {k: pltpu.make_async_copy(part(*k), out.at[k[1], place, k[0]], go.at[*k]) for k in blocks}
    for k in blocks:
        inward[k].start()
    high, low = halves(matrix[...])
    for t in range(strips):
        for d in range(rows):
            inward[t, d].wait()
        for j in range(4):
            wide[:, j * 128 : j * 128 + 128] = line.at[t][pl.ds(j, species, stride=4), :]
        value = wide[...]
        top, rest = halves(value)
        total = jnp.dot(high, top, preferred_element_type=F32)
        total += jnp.dot(high, rest, preferred_element_type=F32)
        total += jnp.dot(low, top, preferred_element_type=F32)
        wide[...] = value + total
        for j in range(4):
            line.at[t][pl.ds(j, species, stride=4), :] = wide[:, j * 128 : j * 128 + 128]
        for d in range(rows):
            outward[t, d].start()
    for k in blocks:
        outward[k].wait()


def prepare(lm, pbl, land, rates, keep, weven, wodd):
    ny = lm.shape[1]
    kinds = lax.broadcasted_iota(jnp.int32, (rates.shape[1], ny), 0)
    levels = lax.broadcasted_iota(jnp.int32, (8, ny), 0)
    evens = 2 * lax.broadcasted_iota(jnp.int32, (4, ny), 0)
    for r in range(8):
        top = pbl[r : r + 1, :]
        mass = lm[pl.ds(r, 8, stride=8), :]
        total = jnp.sum(jnp.where(levels < top, mass, 0.0), axis=0, keepdims=True)
        scale = 1.0 / total
        even = jnp.where(evens < top, lm[pl.ds(r, 4, stride=16), :], 0.0) * scale
        odd = jnp.where(evens + 1 < top, lm[pl.ds(8 + r, 4, stride=16), :], 0.0) * scale
        weven[r, 0:4, :] = even
        weven[r, 4:8, :] = even
        wodd[r, 0:4, :] = odd
        wodd[r, 4:8, :] = odd
        onehot = (kinds == land[r : r + 1, :]).astype(F32)
        loss = jnp.dot(
            rates[...], onehot, precision=lax.Precision.HIGHEST, preferred_element_type=F32
        )
        keep[r, 0] = jnp.exp(-loss)


def finish(even, odd, keep, weven, wodd, pbl, lm, out, dep, flux):
    t = pl.program_id(0)
    ny = even.shape[3]
    width = even.shape[2]
    sub = lax.broadcasted_iota(jnp.int32, (8, ny), 0)
    level = 2 * (sub % 4)
    first = sub % 2 == 0
    low = sub % 4 < 2
    for r in range(8):
        top = pbl[r : r + 1, :]
        for i in range(width // 8):
            at = slice(i * 8, i * 8 + 8)
            a, b = even[r, t, at, :], odd[r, 0, at, :]
            total = weven[r] * a + wodd[r] * b
            total += jnp.where(first, pltpu.roll(total, 7, 0), pltpu.roll(total, 1, 0))
            total += jnp.where(low, pltpu.roll(total, 6, 0), pltpu.roll(total, 2, 0))
            a = jnp.where(level < top, total, a)
            b = jnp.where(level + 1 < top, total, b)
            kept = a * keep[r, 0, at, :]
            flux[at, :] = (a - kept) * lm[r : r + 1, :]
            out[pl.ds(i * 128 + r, 8, stride=16), :] = kept
            out[pl.ds(i * 128 + 8 + r, 8, stride=16), :] = b
        count = width // 4
        dep[pl.ds(r, count, stride=8), :] = flux[pl.ds(0, count, stride=4), :]


def on_device(tracers, courant, layer_mass, pbl_top, land_type, rates, coupling):
    own_species, _, rows, ny = tracers.shape
    species = coupling.shape[0]
    width = own_species * 4
    sds = jax.ShapeDtypeStruct
    n_space = lax.axis_size("space")
    up_pairs = [(i, i + 1) for i in range(n_space - 1)]
    down_pairs = [(j, i) for i, j in up_pairs]
    split = tracers.reshape(own_species, 4, 2, rows, ny)
    cf = courant.reshape(-1, ny)
    lm = layer_mass.reshape(-1, ny)
    valid = (lax.axis_index("space") > 0).astype(F32).reshape(1, 1)

    strips = ny // 128
    group = sds((rows, strips, width, 128), F32)
    edge = sds((strips, HALO * width + 64, 128), F32)
    speeds = sds((2, 2, rows, 8, ny), F32)

    def strip(*shape):
        return pl.BlockSpec((*shape, 128), lambda t: (0,) * len(shape) + (t,))

    def columns(count):
        return pl.BlockSpec((count, 1, width, 128), lambda t: (0, t, 0, 0))

    ends = pl.BlockSpec((1, HALO * width + 64, 128), lambda t: (t, 0, 0))

    def level_group(parity):
        shape = (own_species, 4, 1, rows, 128)
        return pl.BlockSpec(shape, lambda t: (0, 0, parity, 0, t))

    even, send_up, send_down, speeds = call(
        pack_even,
        (group, edge, edge, speeds),
        grid=(strips,),
        in_specs=[level_group(0), strip(cf.shape[0])],
        out_specs=[
            columns(rows),
            ends,
            ends,
            strip(2, 2, rows, 8),
        ],
    )(split, cf)
    up = lax.ppermute(send_up, "space", up_pairs)
    down = lax.ppermute(send_down, "space", down_pairs)
    odd = call(
        pack_odd,
        group,
        grid=(strips,),
        in_specs=[level_group(1)],
        out_specs=columns(rows),
    )(split)

    def exchange(a):
        return lax.all_to_all(a, "spec", split_axis=0, concat_axis=0, tiled=True)

    pair = far_shape((rows, 2, strips, width, 128))

    whole = pl.BlockSpec(memory_space=pltpu.VMEM)
    anywhere = pl.BlockSpec(memory_space=pl.ANY)
    far_spec = anywhere if INTERPRET else pl.BlockSpec(memory_space=pltpu.HBM)

    def coupled(a, index, shape, place, *into):
        return call(
            functools.partial(couple, index, place),
            shape,
            grant=GRANT,
            in_specs=[anywhere, whole] + [far_spec] * len(into),
            out_specs=far_spec,
            scratch_shapes=[
                pltpu.VMEM((species, 512), F32),
                pltpu.VMEM((strips, species * 4, 128), F32),
                pltpu.SemaphoreType.DMA((strips, rows)),
                pltpu.SemaphoreType.DMA((strips, rows)),
            ],
            input_output_aliases={2: 0} if into else {},
        )(a, coupling, *into)

    cup, cdown = up, down

    def transported(parity, a, index, shape, before, after):
        return call(
            functools.partial(transport, parity, index),
            shape,
            grant=GRANT,
            in_specs=[anywhere] * 6 + [pl.BlockSpec(memory_space=pltpu.SMEM)],
            out_specs=far_spec,
            scratch_shapes=[
                pltpu.VMEM((20, strips, width, 128), F32),
                pltpu.VMEM((2, 16, 8, ny), F32),
                pltpu.VMEM((2, strips, 64, 128), F32),
                pltpu.VMEM((14, TAPS, 8, ny), F32),
                pltpu.VMEM((14, TAPS, 8, ny), F32),
                pltpu.VMEM((14, 3, 8, ny), F32),
                pltpu.VMEM((rows, strips, width, 128), F32),
                pltpu.SemaphoreType.DMA((16,)),
            ],
        )(far(a) if index == 0 else a, before, after, cup, cdown, far(speeds), valid)

    start = lax.axis_index("spec") * own_species
    mine = lax.dynamic_slice_in_dim(rates, start, own_species, 1).T
    kinds = mine.shape[1]
    mine = jnp.pad(mine[:, None], ((0, 0), (0, 3), (0, 16 - kinds))).reshape(width, 16)
    tile = sds((rows, 8, ny), F32)
    keep, weven, wodd = call(
        prepare,
        (group, tile, tile),
        grid=(strips,),
        in_specs=[
            strip(lm.shape[0]),
            strip(rows),
            strip(rows),
            pl.BlockSpec(mine.shape, lambda t: (0, 0)),
        ],
        out_specs=[columns(rows), strip(rows, 8), strip(rows, 8)],
    )(lm, pbl_top, land_type, mine)

    single = far_shape((rows, 1, strips, width, 128))

    odd = exchange(odd)
    both = transported(0, even[:, None], 0, pair, up, down)
    both = coupled(odd[:, None], 0, pair, 1, both)
    both = exchange(both)
    up = lax.ppermute(both[2:, 1], "space", up_pairs)
    down = lax.ppermute(both[:HALO, 1], "space", down_pairs)
    even = coupled(both, 0, single, 0)
    even = exchange(even)[:, 0]
    odd = transported(1, both, 1, single, up, down)[:, 0]

    updated, deposited = call(
        finish,
        (sds((tracers.size // ny, ny), F32), sds((own_species * rows, ny), F32)),
        grid=(strips,),
        in_specs=[whole] + [columns(rows)] * 2 + [strip(rows, 8)] * 2 + [strip(rows)] * 2,
        out_specs=[strip(tracers.size // ny), strip(own_species * rows)],
        scratch_shapes=[pltpu.VMEM((width, 128), F32)],
    )(near(even), odd, keep, weven, wodd, pbl_top, lm)
    return (updated.reshape(tracers.shape), deposited.reshape(own_species, rows, ny))


def solution(mesh):
    return jax.shard_map(
        on_device,
        mesh=mesh,
        in_specs=(
            P("spec", None, "space", None),
            P(None, None, "space", None),
            P(None, "space", None),
            P("space", None),
            P("space", None),
            P(),
            P(),
        ),
        out_specs=(P("spec", None, "space", None), P("spec", "space", None)),
        check_vma=False,
    )
```

```python
import functools

import jax
import jax.numpy as jnp
from jax import lax
from jax.experimental import pallas as pl
from jax.experimental.pallas import tpu as pltpu
from jax.sharding import PartitionSpec as P


INTERPRET = False
F32 = jnp.float32
BF16 = jnp.bfloat16
TAPS = 7
GRANT = 48 << 20
HALO = 6


def near(array):
    return array if INTERPRET else pltpu.with_memory_space_constraint(array, pltpu.VMEM)


def far(array):
    return array if INTERPRET else pltpu.with_memory_space_constraint(array, pltpu.HBM)


def far_shape(shape):
    return jax.ShapeDtypeStruct(shape, F32) if INTERPRET else pltpu.HBM(shape, F32)


def call(body, out_shape, grant=None, **kw):
    params = pltpu.CompilerParams(vmem_limit_bytes=grant)
    return pl.pallas_call(
        body, out_shape=out_shape, interpret=INTERPRET, compiler_params=params, **kw
    )


def pack(x, y, cf, up, down, speeds, odd):
    width = odd.shape[2]
    x = x.reshape(width * 8, 128)
    y = y.reshape(width * 8, 128)
    for r in range(8):
        for i in range(width // 8):
            value = x[pl.ds(i * 64 + r, 8, stride=8), :]
            if r >= 2:
                at = (r - 2) * width + i * 8
                up[0, at : at + 8, :] = value
            if r < 6:
                at = r * width + i * 8
                down[0, at : at + 8, :] = value
            odd[r, 0, i * 8 : i * 8 + 8, :] = y[pl.ds(i * 64 + r, 8, stride=8), :]
    for d in range(2):
        for parity in range(2):
            for row in range(4):
                at = HALO * width + ((d * 2 + parity) * 4 + row) * 4
                start = d * 64 + parity * 8 + row
                before = cf[pl.ds(start, 4, stride=16), :]
                after = cf[pl.ds(start + 4, 4, stride=16), :]
                down[0, at : at + 4, :] = before
                up[0, at : at + 4, :] = after
                for half in (slice(0, 4), slice(4, 8)):
                    speeds[parity, d, row, half, :] = before
                    speeds[parity, d, row + 4, half, :] = after


def flux_taps(c):
    u = jnp.abs(c)
    square = u * u
    edge = c * (1.0 - u) * (1.0 - u)
    other = square * (1.0 - u)
    centre = square * (3.0 - 2.0 * u)
    ahead = c >= 0.0
    below = jnp.where(ahead, -other, 0.0)
    above = jnp.where(ahead, 0.0, other)
    lower = jnp.where(ahead, centre, 0.0)
    upper = jnp.where(ahead, 0.0, -centre)
    a, b = 7.0 / 12.0, 1.0 / 12.0
    return (
        -b * below,
        a * below - b * edge,
        a * (edge + below) - b * above + lower,
        a * (edge + above) - b * below + upper,
        a * above - b * edge,
        -b * above,
    )


def cell_taps(low, high):
    return (
        low[0],
        low[1] - high[0],
        low[2] - high[1],
        1.0 + low[3] - high[2],
        low[4] - high[3],
        low[5] - high[4],
        -high[5],
    )


def transport(
    parity, own, extra, up, down, cup, cdown, cf, valid, out, q, c, ends, wx, wy, mid, new, sems
):
    strips, width = out.shape[2], out.shape[3]
    ny = strips * 128
    group = 24
    packed = parity == 0
    tail = pl.ds(HALO * width, 64)
    moves = [
        pltpu.make_async_copy(cf.at[parity], c.at[:, pl.ds(4, 8)], sems.at[0]),
        pltpu.make_async_copy(cup.at[:, tail], ends.at[0], sems.at[1]),
        pltpu.make_async_copy(cdown.at[:, tail], ends.at[1], sems.at[2]),
    ]
    if packed:
        for row in range(8):
            at = row if row < HALO else row - 2
            source = own if row < HALO else extra
            move = source.at[:, pl.ds(at * width, width)], q.at[HALO + row], sems.at[15 + row]
            moves.append(pltpu.make_async_copy(*move))
    else:
        moves.append(pltpu.make_async_copy(own.at[:, 1], q.at[pl.ds(HALO, 8)], sems.at[15]))
    for row in range(HALO):
        span = pl.ds(row * width, width)
        before = up.at[:, span] if packed else up.at[row]
        after = down.at[:, span] if packed else down.at[row]
        moves.append(pltpu.make_async_copy(before, q.at[row], sems.at[3 + row]))
        moves.append(pltpu.make_async_copy(after, q.at[HALO + 8 + row], sems.at[9 + row]))
    for move in moves:
        move.start()
    for move in moves[:3]:
        move.wait()
    for d in range(2):
        for row in range(4):
            at = ((d * 2 + parity) * 4 + row) * 4
            for t in range(strips):
                cols = slice(t * 128, t * 128 + 128)
                for half in (slice(0, 4), slice(4, 8)):
                    c[d, row, half, cols] = ends[0, t, at : at + 4, :]
                    c[d, row + 12, half, cols] = ends[1, t, at : at + 4, :]
    lane = lax.broadcasted_iota(jnp.int32, (8, ny), 1)
    inside = valid[0, 0]

    def weights(row, carry):
        keep = jnp.where(row < 3, inside, 1.0)
        taps = cell_taps(flux_taps(c[0, row + 1]), flux_taps(c[0, row + 2]))
        for k, w in enumerate(taps):
            wx[row, k] = w * keep
        speed = c[1, row + 1]
        low = flux_taps(speed)
        high = flux_taps(jnp.where(lane == ny - 1, 0.0, pltpu.roll(speed, ny - 1, 1)))
        for k, w in enumerate(cell_taps(low, high)):
            shift = k - 3
            w = jnp.where((lane + shift >= 0) & (lane + shift < ny), w, 0.0)
            wy[row, k] = w
        return carry

    lax.fori_loop(0, 14, weights, 0)
    for move in moves[3:]:
        move.wait()
    parts = range(group // 8)

    def across(values, row):
        w = wy[row, 3]
        totals = [w * v for v in values]
        for shift in (1, 2, 3):
            w = wy[row, 3 + shift]
            totals = [t + w * pltpu.roll(v, ny - shift, 1) for t, v in zip(totals, values)]
            w = wy[row, 3 - shift]
            totals = [t + w * pltpu.roll(v, shift, 1) for t, v in zip(totals, values)]
        return totals

    def along(read, row, base):
        done = [[] for _ in parts]
        for t in range(strips):
            cols = slice(t * 128, t * 128 + 128)
            w = wx[row, 0, :, cols]
            totals = [w * read(base, t, u) for u in parts]
            for k in range(1, TAPS):
                w = wx[row, k, :, cols]
                totals = [v + w * read(base + k, t, u) for u, v in enumerate(totals)]
            for u in parts:
                done[u].append(totals[u])
        return [jnp.concatenate(pieces, axis=1) for pieces in done]

    def back(i):
        span = pl.ds(pl.multiple_of(i * group, 8), group)
        return pltpu.make_async_copy(new.at[:, :, span], out.at[:, 0, :, span], sems.at[i])

    def block(i, carry):
        places = [pl.multiple_of(i * group + u * 8, 8) for u in parts]

        def first(row, t, u):
            return q[row, t, pl.ds(places[u], 8), :]

        def second(row, t, u):
            return mid[row, u, :, t * 128 : t * 128 + 128]

        for row in range(14):
            for u, v in enumerate(across(along(first, row, row), row)):
                mid[row, u] = v
        for row in range(8):
            for u, v in enumerate(across(along(second, row + 3, row), row + 3)):
                for t in range(strips):
                    new[row, t, pl.ds(places[u], 8), :] = v[:, t * 128 : t * 128 + 128]
        back(i).start()
        return carry

    lax.fori_loop(0, width // group, block, 0)
    for i in range(width // group):
        back(i).wait()


def halves(value):
    top = value.astype(BF16)
    return top, (value - top.astype(F32)).astype(BF16)


def couple(index, place, x, matrix, *refs):
    out, wide, line, come, go = refs[-5:]
    species = matrix.shape[0]
    rows, strips, width = x.shape[0], x.shape[2], x.shape[3]

    def part(t, d):
        return line.at[t, pl.ds(d * width, width)]

    blocks = [(t, d) for t in range(strips) for d in range(rows)]
    inward = {k: pltpu.make_async_copy(x.at[k[1], index, k[0]], part(*k), come.at[*k]) for k in blocks}
    outward = {k: pltpu.make_async_copy(part(*k), out.at[k[1], place, k[0]], go.at[*k]) for k in blocks}
    for k in blocks:
        inward[k].start()
    high, low = halves(matrix[...])
    for t in range(strips):
        for d in range(rows):
            inward[t, d].wait()
        for j in range(4):
            wide[:, j * 128 : j * 128 + 128] = line.at[t][pl.ds(j, species, stride=4), :]
        value = wide[...]
        top, rest = halves(value)
        total = jnp.dot(high, top, preferred_element_type=F32)
        total += jnp.dot(high, rest, preferred_element_type=F32)
        total += jnp.dot(low, top, preferred_element_type=F32)
        wide[...] = value + total
        for j in range(4):
            line.at[t][pl.ds(j, species, stride=4), :] = wide[:, j * 128 : j * 128 + 128]
        for d in range(rows):
            outward[t, d].start()
    for k in blocks:
        outward[k].wait()


def prepare(lm, pbl, land, rates, keep, weven, wodd):
    ny = lm.shape[1]
    kinds = lax.broadcasted_iota(jnp.int32, (rates.shape[1], ny), 0)
    levels = lax.broadcasted_iota(jnp.int32, (8, ny), 0)
    evens = 2 * lax.broadcasted_iota(jnp.int32, (4, ny), 0)
    for r in range(8):
        top = pbl[r : r + 1, :]
        mass = lm[pl.ds(r, 8, stride=8), :]
        total = jnp.sum(jnp.where(levels < top, mass, 0.0), axis=0, keepdims=True)
        scale = 1.0 / total
        even = jnp.where(evens < top, lm[pl.ds(r, 4, stride=16), :], 0.0) * scale
        odd = jnp.where(evens + 1 < top, lm[pl.ds(8 + r, 4, stride=16), :], 0.0) * scale
        weven[r, 0:4, :] = even
        weven[r, 4:8, :] = even
        wodd[r, 0:4, :] = odd
        wodd[r, 4:8, :] = odd
        onehot = (kinds == land[r : r + 1, :]).astype(F32)
        loss = jnp.dot(
            rates[...], onehot, precision=lax.Precision.HIGHEST, preferred_element_type=F32
        )
        keep[r, 0] = jnp.exp(-loss)


def finish(even, odd, keep, weven, wodd, pbl, lm, out, dep, flux):
    t = pl.program_id(0)
    ny = even.shape[3]
    width = even.shape[2]
    sub = lax.broadcasted_iota(jnp.int32, (8, ny), 0)
    level = 2 * (sub % 4)
    first = sub % 2 == 0
    low = sub % 4 < 2
    for r in range(8):
        top = pbl[r : r + 1, :]
        for i in range(width // 8):
            at = slice(i * 8, i * 8 + 8)
            a, b = even[r, t, at, :], odd[r, 0, at, :]
            total = weven[r] * a + wodd[r] * b
            total += jnp.where(first, pltpu.roll(total, 7, 0), pltpu.roll(total, 1, 0))
            total += jnp.where(low, pltpu.roll(total, 6, 0), pltpu.roll(total, 2, 0))
            a = jnp.where(level < top, total, a)
            b = jnp.where(level + 1 < top, total, b)
            kept = a * keep[r, 0, at, :]
            flux[at, :] = (a - kept) * lm[r : r + 1, :]
            out[pl.ds(i * 128 + r, 8, stride=16), :] = kept
            out[pl.ds(i * 128 + 8 + r, 8, stride=16), :] = b
        count = width // 4
        dep[pl.ds(r, count, stride=8), :] = flux[pl.ds(0, count, stride=4), :]


def on_device(tracers, courant, layer_mass, pbl_top, land_type, rates, coupling):
    own_species, _, rows, ny = tracers.shape
    species = coupling.shape[0]
    width = own_species * 4
    sds = jax.ShapeDtypeStruct
    n_space = lax.axis_size("space")
    up_pairs = [(i, i + 1) for i in range(n_space - 1)]
    down_pairs = [(j, i) for i, j in up_pairs]
    split = tracers.reshape(own_species, 4, 2, rows, ny)
    cf = courant.reshape(-1, ny)
    lm = layer_mass.reshape(-1, ny)
    valid = (lax.axis_index("space") > 0).astype(F32).reshape(1, 1)

    strips = ny // 128
    group = sds((rows, strips, width, 128), F32)
    edge = sds((strips, HALO * width + 64, 128), F32)
    speeds = sds((2, 2, rows, 8, ny), F32)

    def strip(*shape):
        return pl.BlockSpec((*shape, 128), lambda t: (0,) * len(shape) + (t,))

    def columns(count):
        return pl.BlockSpec((count, 1, width, 128), lambda t: (0, t, 0, 0))

    ends = pl.BlockSpec((1, HALO * width + 64, 128), lambda t: (t, 0, 0))

    def level_group(parity):
        shape = (own_species, 4, 1, rows, 128)
        return pl.BlockSpec(shape, lambda t: (0, 0, parity, 0, t))

    send_up, send_down, speeds, odd = call(
        pack,
        (edge, edge, speeds, group),
        grid=(strips,),
        in_specs=[level_group(0), level_group(1), strip(cf.shape[0])],
        out_specs=[ends, ends, strip(2, 2, rows, 8), columns(rows)],
    )(split, split, cf)
    up = lax.ppermute(send_up, "space", up_pairs)
    down = lax.ppermute(send_down, "space", down_pairs)

    def exchange(a):
        return lax.all_to_all(a, "spec", split_axis=0, concat_axis=0, tiled=True)

    pair = far_shape((rows, 2, strips, width, 128))

    whole = pl.BlockSpec(memory_space=pltpu.VMEM)
    anywhere = pl.BlockSpec(memory_space=pl.ANY)
    far_spec = anywhere if INTERPRET else pl.BlockSpec(memory_space=pltpu.HBM)

    def coupled(a, index, shape, place, *into):
        return call(
            functools.partial(couple, index, place),
            shape,
            grant=GRANT,
            in_specs=[anywhere, whole] + [far_spec] * len(into),
            out_specs=far_spec,
            scratch_shapes=[
                pltpu.VMEM((species, 512), F32),
                pltpu.VMEM((strips, species * 4, 128), F32),
                pltpu.SemaphoreType.DMA((strips, rows)),
                pltpu.SemaphoreType.DMA((strips, rows)),
            ],
            input_output_aliases={2: 0} if into else {},
        )(a, coupling, *into)

    cup, cdown = up, down

    def transported(parity, a, extra, shape, before, after):
        return call(
            functools.partial(transport, parity),
            shape,
            grant=GRANT,
            in_specs=[anywhere] * 7 + [pl.BlockSpec(memory_space=pltpu.SMEM)],
            out_specs=far_spec,
            scratch_shapes=[
                pltpu.VMEM((20, strips, width, 128), F32),
                pltpu.VMEM((2, 16, 8, ny), F32),
                pltpu.VMEM((2, strips, 64, 128), F32),
                pltpu.VMEM((14, TAPS, 8, ny), F32),
                pltpu.VMEM((14, TAPS, 8, ny), F32),
                pltpu.VMEM((14, 3, 8, ny), F32),
                pltpu.VMEM((rows, strips, width, 128), F32),
                pltpu.SemaphoreType.DMA((23,)),
            ],
        )(a, extra, before, after, cup, cdown, far(speeds), valid)

    start = lax.axis_index("spec") * own_species
    mine = lax.dynamic_slice_in_dim(rates, start, own_species, 1).T
    kinds = mine.shape[1]
    mine = jnp.pad(mine[:, None], ((0, 0), (0, 3), (0, 16 - kinds))).reshape(width, 16)
    tile = sds((rows, 8, ny), F32)
    keep, weven, wodd = call(
        prepare,
        (group, tile, tile),
        grid=(strips,),
        in_specs=[
            strip(lm.shape[0]),
            strip(rows),
            strip(rows),
            pl.BlockSpec(mine.shape, lambda t: (0, 0)),
        ],
        out_specs=[columns(rows), strip(rows, 8), strip(rows, 8)],
    )(lm, pbl_top, land_type, mine)

    single = far_shape((rows, 1, strips, width, 128))

    odd = exchange(odd)
    both = transported(0, far(send_down), far(send_up), pair, up, down)
    both = coupled(odd[:, None], 0, pair, 1, both)
    both = exchange(both)
    up = lax.ppermute(both[2:, 1], "space", up_pairs)
    down = lax.ppermute(both[:HALO, 1], "space", down_pairs)
    even = coupled(both, 0, single, 0)
    even = exchange(even)[:, 0]
    odd = transported(1, both, valid, single, up, down)[:, 0]

    updated, deposited = call(
        finish,
        (sds((tracers.size // ny, ny), F32), sds((own_species * rows, ny), F32)),
        grid=(strips,),
        in_specs=[whole] + [columns(rows)] * 2 + [strip(rows, 8)] * 2 + [strip(rows)] * 2,
        out_specs=[strip(tracers.size // ny), strip(own_species * rows)],
        scratch_shapes=[pltpu.VMEM((width, 128), F32)],
    )(near(even), odd, keep, weven, wodd, pbl_top, lm)
    return (updated.reshape(tracers.shape), deposited.reshape(own_species, rows, ny))


def solution(mesh):
    return jax.shard_map(
        on_device,
        mesh=mesh,
        in_specs=(
            P("spec", None, "space", None),
            P(None, None, "space", None),
            P(None, "space", None),
            P("space", None),
            P("space", None),
            P(),
            P(),
        ),
        out_specs=(P("spec", None, "space", None), P("spec", "space", None)),
        check_vma=False,
    )
```

```python
import functools

import jax
import jax.numpy as jnp
from jax import lax
from jax.experimental import pallas as pl
from jax.experimental.pallas import tpu as pltpu
from jax.sharding import PartitionSpec as P


INTERPRET = False
F32 = jnp.float32
BF16 = jnp.bfloat16
TAPS = 7
GRANT = 48 << 20
HALO = 6


def near(array):
    return array if INTERPRET else pltpu.with_memory_space_constraint(array, pltpu.VMEM)


def far(array):
    return array if INTERPRET else pltpu.with_memory_space_constraint(array, pltpu.HBM)


def far_shape(shape):
    return jax.ShapeDtypeStruct(shape, F32) if INTERPRET else pltpu.HBM(shape, F32)


def call(body, out_shape, grant=None, **kw):
    params = pltpu.CompilerParams(vmem_limit_bytes=grant)
    return pl.pallas_call(
        body, out_shape=out_shape, interpret=INTERPRET, compiler_params=params, **kw
    )


def pack_even(x, cf, up, down, speeds):
    width = x.shape[0] * 4
    x = x.reshape(width * 8, 128)
    for r in range(8):
        for i in range(width // 8):
            value = x[pl.ds(i * 64 + r, 8, stride=8), :]
            if r >= 2:
                at = (r - 2) * width + i * 8
                up[0, at : at + 8, :] = value
            if r < 6:
                at = r * width + i * 8
                down[0, at : at + 8, :] = value
    for d in range(2):
        for parity in range(2):
            for row in range(4):
                at = HALO * width + ((d * 2 + parity) * 4 + row) * 4
                start = d * 64 + parity * 8 + row
                before = cf[pl.ds(start, 4, stride=16), :]
                after = cf[pl.ds(start + 4, 4, stride=16), :]
                down[0, at : at + 4, :] = before
                up[0, at : at + 4, :] = after
                for half in (slice(0, 4), slice(4, 8)):
                    speeds[parity, d, row, half, :] = before
                    speeds[parity, d, row + 4, half, :] = after


def pack_odd(x, own):
    x = x.reshape(own.shape[2] * 8, 128)
    for r in range(8):
        for i in range(own.shape[2] // 8):
            own[r, 0, i * 8 : i * 8 + 8, :] = x[pl.ds(i * 64 + r, 8, stride=8), :]


def flux_taps(c):
    u = jnp.abs(c)
    square = u * u
    edge = c * (1.0 - u) * (1.0 - u)
    other = square * (1.0 - u)
    centre = square * (3.0 - 2.0 * u)
    ahead = c >= 0.0
    below = jnp.where(ahead, -other, 0.0)
    above = jnp.where(ahead, 0.0, other)
    lower = jnp.where(ahead, centre, 0.0)
    upper = jnp.where(ahead, 0.0, -centre)
    a, b = 7.0 / 12.0, 1.0 / 12.0
    return (
        -b * below,
        a * below - b * edge,
        a * (edge + below) - b * above + lower,
        a * (edge + above) - b * below + upper,
        a * above - b * edge,
        -b * above,
    )


def cell_taps(low, high):
    return (
        low[0],
        low[1] - high[0],
        low[2] - high[1],
        1.0 + low[3] - high[2],
        low[4] - high[3],
        low[5] - high[4],
        -high[5],
    )


def transport(
    parity, own, extra, up, down, cup, cdown, cf, valid, out, q, c, ends, wx, wy, mid, new, sems
):
    strips, width = out.shape[2], out.shape[3]
    ny = strips * 128
    group = 24
    packed = parity == 0
    tail = pl.ds(HALO * width, 64)
    moves = [
        pltpu.make_async_copy(cf.at[parity], c.at[:, pl.ds(4, 8)], sems.at[0]),
        pltpu.make_async_copy(cup.at[:, tail], ends.at[0], sems.at[1]),
        pltpu.make_async_copy(cdown.at[:, tail], ends.at[1], sems.at[2]),
    ]
    if packed:
        for row in range(8):
            at = row if row < HALO else row - 2
            source = own if row < HALO else extra
            move = source.at[:, pl.ds(at * width, width)], q.at[HALO + row], sems.at[15 + row]
            moves.append(pltpu.make_async_copy(*move))
    else:
        moves.append(pltpu.make_async_copy(own.at[:, 1], q.at[pl.ds(HALO, 8)], sems.at[15]))
    for row in range(HALO):
        span = pl.ds(row * width, width)
        before = up.at[:, span] if packed else up.at[row]
        after = down.at[:, span] if packed else down.at[row]
        moves.append(pltpu.make_async_copy(before, q.at[row], sems.at[3 + row]))
        moves.append(pltpu.make_async_copy(after, q.at[HALO + 8 + row], sems.at[9 + row]))
    for move in moves:
        move.start()
    for move in moves[:3]:
        move.wait()
    for d in range(2):
        for row in range(4):
            at = ((d * 2 + parity) * 4 + row) * 4
            for t in range(strips):
                cols = slice(t * 128, t * 128 + 128)
                for half in (slice(0, 4), slice(4, 8)):
                    c[d, row, half, cols] = ends[0, t, at : at + 4, :]
                    c[d, row + 12, half, cols] = ends[1, t, at : at + 4, :]
    lane = lax.broadcasted_iota(jnp.int32, (8, ny), 1)
    inside = valid[0, 0]

    def weights(row, carry):
        keep = jnp.where(row < 3, inside, 1.0)
        taps = cell_taps(flux_taps(c[0, row + 1]), flux_taps(c[0, row + 2]))
        for k, w in enumerate(taps):
            wx[row, k] = w * keep
        speed = c[1, row + 1]
        low = flux_taps(speed)
        high = flux_taps(jnp.where(lane == ny - 1, 0.0, pltpu.roll(speed, ny - 1, 1)))
        for k, w in enumerate(cell_taps(low, high)):
            shift = k - 3
            w = jnp.where((lane + shift >= 0) & (lane + shift < ny), w, 0.0)
            wy[row, k] = w
        return carry

    lax.fori_loop(0, 14, weights, 0)
    for move in moves[3:]:
        move.wait()
    parts = range(group // 8)

    def across(values, row):
        w = wy[row, 3]
        totals = [w * v for v in values]
        for shift in (1, 2, 3):
            w = wy[row, 3 + shift]
            totals = [t + w * pltpu.roll(v, ny - shift, 1) for t, v in zip(totals, values)]
            w = wy[row, 3 - shift]
            totals = [t + w * pltpu.roll(v, shift, 1) for t, v in zip(totals, values)]
        return totals

    def along(read, row, base):
        done = [[] for _ in parts]
        for t in range(strips):
            cols = slice(t * 128, t * 128 + 128)
            w = wx[row, 0, :, cols]
            totals = [w * read(base, t, u) for u in parts]
            for k in range(1, TAPS):
                w = wx[row, k, :, cols]
                totals = [v + w * read(base + k, t, u) for u, v in enumerate(totals)]
            for u in parts:
                done[u].append(totals[u])
        return [jnp.concatenate(pieces, axis=1) for pieces in done]

    def back(i):
        span = pl.ds(pl.multiple_of(i * group, 8), group)
        return pltpu.make_async_copy(new.at[:, :, span], out.at[:, 0, :, span], sems.at[i])

    def block(i, carry):
        places = [pl.multiple_of(i * group + u * 8, 8) for u in parts]

        def first(row, t, u):
            return q[row, t, pl.ds(places[u], 8), :]

        def second(row, t, u):
            return mid[row, u, :, t * 128 : t * 128 + 128]

        for row in range(14):
            for u, v in enumerate(across(along(first, row, row), row)):
                mid[row, u] = v
        for row in range(8):
            for u, v in enumerate(across(along(second, row + 3, row), row + 3)):
                for t in range(strips):
                    new[row, t, pl.ds(places[u], 8), :] = v[:, t * 128 : t * 128 + 128]
        back(i).start()
        return carry

    lax.fori_loop(0, width // group, block, 0)
    for i in range(width // group):
        back(i).wait()


def halves(value):
    top = value.astype(BF16)
    return top, (value - top.astype(F32)).astype(BF16)


def couple(index, place, x, matrix, *refs):
    out, wide, line, come, go = refs[-5:]
    species = matrix.shape[0]
    rows, strips, width = x.shape[0], x.shape[2], x.shape[3]

    def part(t, d):
        return line.at[t, pl.ds(d * width, width)]

    blocks = [(t, d) for t in range(strips) for d in range(rows)]
    inward = {k: pltpu.make_async_copy(x.at[k[1], index, k[0]], part(*k), come.at[*k]) for k in blocks}
    outward = {k: pltpu.make_async_copy(part(*k), out.at[k[1], place, k[0]], go.at[*k]) for k in blocks}
    for k in blocks:
        inward[k].start()
    high, low = halves(matrix[...])
    for t in range(strips):
        for d in range(rows):
            inward[t, d].wait()
        for j in range(4):
            wide[:, j * 128 : j * 128 + 128] = line.at[t][pl.ds(j, species, stride=4), :]
        value = wide[...]
        top, rest = halves(value)
        total = jnp.dot(high, top, preferred_element_type=F32)
        total += jnp.dot(high, rest, preferred_element_type=F32)
        total += jnp.dot(low, top, preferred_element_type=F32)
        wide[...] = value + total
        for j in range(4):
            line.at[t][pl.ds(j, species, stride=4), :] = wide[:, j * 128 : j * 128 + 128]
        for d in range(rows):
            outward[t, d].start()
    for k in blocks:
        outward[k].wait()


def prepare(lm, pbl, land, rates, keep, weven, wodd):
    ny = lm.shape[1]
    kinds = lax.broadcasted_iota(jnp.int32, (rates.shape[1], ny), 0)
    levels = lax.broadcasted_iota(jnp.int32, (8, ny), 0)
    evens = 2 * lax.broadcasted_iota(jnp.int32, (4, ny), 0)
    for r in range(8):
        top = pbl[r : r + 1, :]
        mass = lm[pl.ds(r, 8, stride=8), :]
        total = jnp.sum(jnp.where(levels < top, mass, 0.0), axis=0, keepdims=True)
        scale = 1.0 / total
        even = jnp.where(evens < top, lm[pl.ds(r, 4, stride=16), :], 0.0) * scale
        odd = jnp.where(evens + 1 < top, lm[pl.ds(8 + r, 4, stride=16), :], 0.0) * scale
        weven[r, 0:4, :] = even
        weven[r, 4:8, :] = even
        wodd[r, 0:4, :] = odd
        wodd[r, 4:8, :] = odd
        onehot = (kinds == land[r : r + 1, :]).astype(F32)
        loss = jnp.dot(
            rates[...], onehot, precision=lax.Precision.HIGHEST, preferred_element_type=F32
        )
        keep[r, 0] = jnp.exp(-loss)


def finish(even, odd, keep, weven, wodd, pbl, lm, out, dep, flux):
    t = pl.program_id(0)
    ny = even.shape[3]
    width = even.shape[2]
    sub = lax.broadcasted_iota(jnp.int32, (8, ny), 0)
    level = 2 * (sub % 4)
    first = sub % 2 == 0
    low = sub % 4 < 2
    for r in range(8):
        top = pbl[r : r + 1, :]
        for i in range(width // 8):
            at = slice(i * 8, i * 8 + 8)
            a, b = even[r, t, at, :], odd[r, 0, at, :]
            total = weven[r] * a + wodd[r] * b
            total += jnp.where(first, pltpu.roll(total, 7, 0), pltpu.roll(total, 1, 0))
            total += jnp.where(low, pltpu.roll(total, 6, 0), pltpu.roll(total, 2, 0))
            a = jnp.where(level < top, total, a)
            b = jnp.where(level + 1 < top, total, b)
            kept = a * keep[r, 0, at, :]
            flux[at, :] = (a - kept) * lm[r : r + 1, :]
            out[pl.ds(i * 128 + r, 8, stride=16), :] = kept
            out[pl.ds(i * 128 + 8 + r, 8, stride=16), :] = b
        count = width // 4
        dep[pl.ds(r, count, stride=8), :] = flux[pl.ds(0, count, stride=4), :]


def on_device(tracers, courant, layer_mass, pbl_top, land_type, rates, coupling):
    own_species, _, rows, ny = tracers.shape
    species = coupling.shape[0]
    width = own_species * 4
    sds = jax.ShapeDtypeStruct
    n_space = lax.axis_size("space")
    up_pairs = [(i, i + 1) for i in range(n_space - 1)]
    down_pairs = [(j, i) for i, j in up_pairs]
    split = tracers.reshape(own_species, 4, 2, rows, ny)
    cf = courant.reshape(-1, ny)
    lm = layer_mass.reshape(-1, ny)
    valid = (lax.axis_index("space") > 0).astype(F32).reshape(1, 1)

    strips = ny // 128
    group = sds((rows, strips, width, 128), F32)
    edge = sds((strips, HALO * width + 64, 128), F32)
    speeds = sds((2, 2, rows, 8, ny), F32)

    def strip(*shape):
        return pl.BlockSpec((*shape, 128), lambda t: (0,) * len(shape) + (t,))

    def columns(count):
        return pl.BlockSpec((count, 1, width, 128), lambda t: (0, t, 0, 0))

    ends = pl.BlockSpec((1, HALO * width + 64, 128), lambda t: (t, 0, 0))

    def level_group(parity):
        shape = (own_species, 4, 1, rows, 128)
        return pl.BlockSpec(shape, lambda t: (0, 0, parity, 0, t))

    send_up, send_down, speeds = call(
        pack_even,
        (edge, edge, speeds),
        grid=(strips,),
        in_specs=[level_group(0), strip(cf.shape[0])],
        out_specs=[ends, ends, strip(2, 2, rows, 8)],
    )(split, cf)
    up = lax.ppermute(send_up, "space", up_pairs)
    down = lax.ppermute(send_down, "space", down_pairs)
    odd = call(
        pack_odd,
        group,
        grid=(strips,),
        in_specs=[level_group(1)],
        out_specs=columns(rows),
    )(split)

    def exchange(a):
        return lax.all_to_all(a, "spec", split_axis=0, concat_axis=0, tiled=True)

    pair = far_shape((rows, 2, strips, width, 128))

    whole = pl.BlockSpec(memory_space=pltpu.VMEM)
    anywhere = pl.BlockSpec(memory_space=pl.ANY)
    far_spec = anywhere if INTERPRET else pl.BlockSpec(memory_space=pltpu.HBM)

    def coupled(a, index, shape, place, *into):
        return call(
            functools.partial(couple, index, place),
            shape,
            grant=GRANT,
            in_specs=[anywhere, whole] + [far_spec] * len(into),
            out_specs=far_spec,
            scratch_shapes=[
                pltpu.VMEM((species, 512), F32),
                pltpu.VMEM((strips, species * 4, 128), F32),
                pltpu.SemaphoreType.DMA((strips, rows)),
                pltpu.SemaphoreType.DMA((strips, rows)),
            ],
            input_output_aliases={2: 0} if into else {},
        )(a, coupling, *into)

    cup, cdown = up, down

    def transported(parity, a, extra, shape, before, after):
        return call(
            functools.partial(transport, parity),
            shape,
            grant=GRANT,
            in_specs=[anywhere] * 7 + [pl.BlockSpec(memory_space=pltpu.SMEM)],
            out_specs=far_spec,
            scratch_shapes=[
                pltpu.VMEM((20, strips, width, 128), F32),
                pltpu.VMEM((2, 16, 8, ny), F32),
                pltpu.VMEM((2, strips, 64, 128), F32),
                pltpu.VMEM((14, TAPS, 8, ny), F32),
                pltpu.VMEM((14, TAPS, 8, ny), F32),
                pltpu.VMEM((14, 3, 8, ny), F32),
                pltpu.VMEM((rows, strips, width, 128), F32),
                pltpu.SemaphoreType.DMA((23,)),
            ],
        )(a, extra, before, after, cup, cdown, far(speeds), valid)

    start = lax.axis_index("spec") * own_species
    mine = lax.dynamic_slice_in_dim(rates, start, own_species, 1).T
    kinds = mine.shape[1]
    mine = jnp.pad(mine[:, None], ((0, 0), (0, 3), (0, 16 - kinds))).reshape(width, 16)
    tile = sds((rows, 8, ny), F32)
    keep, weven, wodd = call(
        prepare,
        (group, tile, tile),
        grid=(strips,),
        in_specs=[
            strip(lm.shape[0]),
            strip(rows),
            strip(rows),
            pl.BlockSpec(mine.shape, lambda t: (0, 0)),
        ],
        out_specs=[columns(rows), strip(rows, 8), strip(rows, 8)],
    )(lm, pbl_top, land_type, mine)

    single = far_shape((rows, 1, strips, width, 128))

    odd = exchange(odd)
    both = transported(0, far(send_down), far(send_up), pair, up, down)
    both = coupled(odd[:, None], 0, pair, 1, both)
    both = exchange(both)
    up = lax.ppermute(both[2:, 1], "space", up_pairs)
    down = lax.ppermute(both[:HALO, 1], "space", down_pairs)
    even = coupled(both, 0, single, 0)
    even = exchange(even)[:, 0]
    odd = transported(1, both, valid, single, up, down)[:, 0]

    updated, deposited = call(
        finish,
        (sds((tracers.size // ny, ny), F32), sds((own_species * rows, ny), F32)),
        grid=(strips,),
        in_specs=[whole] + [columns(rows)] * 2 + [strip(rows, 8)] * 2 + [strip(rows)] * 2,
        out_specs=[strip(tracers.size // ny), strip(own_species * rows)],
        scratch_shapes=[pltpu.VMEM((width, 128), F32)],
    )(near(even), odd, keep, weven, wodd, pbl_top, lm)
    return (updated.reshape(tracers.shape), deposited.reshape(own_species, rows, ny))


def solution(mesh):
    return jax.shard_map(
        on_device,
        mesh=mesh,
        in_specs=(
            P("spec", None, "space", None),
            P(None, None, "space", None),
            P(None, "space", None),
            P("space", None),
            P("space", None),
            P(),
            P(),
        ),
        out_specs=(P("spec", None, "space", None), P("spec", "space", None)),
        check_vma=False,
    )
```
